256 devices in a mesh: region: 4 (over z_hi), tile: 64 (over z_lo, y, x, core).
Axes of the slice: x: 4, y: 4, z: 8 (z_hi: 4, z_lo: 2; z = z_hi * 2 + z_lo), core: 2. Of those that a mesh axis runs over, the one named last changes fastest.
Arguments:
- global_field: bfloat16 [70, 512, 1280], P(None, 'tile', 'region'), may hold values from -6 to 6
- regional_state: bfloat16 [256, 99, 64, 128], P(('region', 'tile')), may hold values from -6 to 6
- windows: int32 [8, 4], replicated, may hold values from 0 to 1152, as said below
- longitude_weights: bfloat16 [8, 512, 128], replicated, may hold values from -0.75 to 0.75
- latitude_weights: bfloat16 [8, 512, 64], P('region'), may hold values from -1 to 1
- first_kernel: bfloat16 [3, 3, 96, 169], replicated, may hold values from -0.15625 to 0.15625
- first_bias: float32 [96], replicated, may hold values from -3 to 3
- second_kernel: bfloat16 [3, 3, 96, 96], replicated, may hold values from -0.21875 to 0.21875
- later_conv_bias: float32 [96], replicated, may hold values from -3 to 3
- shortcut_weight: bfloat16 [96, 169], replicated, may hold values from -0.5 to 0.5
Outputs:
- block_output: bfloat16 [256, 96, 64, 128], P(('region', 'tile'))
The draws below stay inside these ranges and needn't reach their ends.
Inputs may be any that keep to these rules, and one draw needn't show every extreme that they name: `windows`: columns per domain: latitude start 0 to 448, latitude rows used 64 // 2 to 64, longitude start 0 to 1152, longitude columns used 128 // 2 to 128; some domain uses all 64 rows and some all 128 columns.
All inputs are finite; a program needn't handle non-finite values.
Results may differ from the reference program's by a relative error of at most 0.0053.
Values may be sent and summed in bfloat16 or wider, within the bound.
No kernel may reach another device: no remote copies, remote signals or barrier semaphores. Data moves between devices by JAX's collectives and lax.ppermute only.
A program may use at most 128 MiB of HBM per device.

```python
import jax
import jax.numpy as jnp
from jax import lax

GCH = 70
SCH = 99
OCH = 96
TCOLS = 4
HY = 64
HX = 128
LAT = 512
LON = 1280
LWIN = 64
KWIN = 128
CIN = 169
DOMAINS = 8
TILES = 256
RY = 512
RX = 512
N_REGION = 4
N_TILE = 64


def draw_windows(key, part):
    subkeys = jax.random.split(key, 5)
    lat_start = jax.random.randint(subkeys[0], (DOMAINS,), 0, LAT - LWIN + 1)
    lat_count = jax.random.randint(subkeys[1], (DOMAINS,), LWIN // 2, LWIN + 1)
    lon_start = jax.random.randint(subkeys[2], (DOMAINS,), 0, LON - KWIN + 1)
    lon_count = jax.random.randint(subkeys[3], (DOMAINS,), KWIN // 2, KWIN + 1)
    fullest = jax.random.randint(subkeys[4], (2,), 0, DOMAINS)
    domain_slots = jnp.arange(DOMAINS)
    lat_count = jnp.where(domain_slots == fullest[0], LWIN, lat_count)
    lon_count = jnp.where(domain_slots == fullest[1], KWIN, lon_count)
    return jnp.stack([lat_start, lat_count, lon_start, lon_count], axis=1).astype(jnp.int32)


def shard_levels(own_key, dims, cuts, low, high):
    def one(axis_at, parts):
        heights = jax.random.uniform(jax.random.fold_in(jax.random.fold_in(own_key, 6), axis_at), (parts,), jnp.float32, low / len(cuts), high / len(cuts))
        return jnp.repeat(jnp.exp(heights), dims[axis_at] // parts).reshape((-1,) + (1,) * (len(dims) - axis_at - 1))

    level = one(*cuts[0])
    for cut in cuts[1:]:
        level = level * one(*cut)
    return level


def scatter_about(own_key, extent, scale, limit, pieces=(), kind=jnp.bfloat16):
    factor_of = shard_levels(own_key, extent, pieces, -0.22, 0.18) if pieces else 1.0
    result = jax.random.normal(own_key, extent, jnp.float32) * scale * factor_of
    return jnp.minimum(jnp.maximum(result, -limit), limit).astype(kind)


def setup_inputs(seed: int = 0) -> dict:
    splits = jax.random.split(jax.random.key(seed), 11)
    global_field = scatter_about(splits[0], (GCH, LAT, LON), 1.0, 6.0, ((1, 64), (2, 4)))
    regional_state = scatter_about(splits[1], (TILES, SCH, HY, HX), 1.0, 6.0, ((0, 256),))
    windows = draw_windows(jax.random.fold_in(splits[10], 71), 0)
    longitude_weights = scatter_about(splits[3], (DOMAINS, RX, KWIN), (KWIN // 2) ** -0.5, 0.75)
    latitude_weights = scatter_about(splits[4], (DOMAINS, RY, LWIN), (LWIN // 2) ** -0.5, 1.0, ((0, 4),))
    first_kernel = scatter_about(splits[5], (3, 3, OCH, CIN), (9 * CIN) ** -0.5, 0.15625)
    first_bias = scatter_about(splits[6], (OCH,), 0.5, 3.0, (), jnp.float32)
    second_kernel = scatter_about(splits[7], (3, 3, OCH, OCH), (9 * OCH) ** -0.5, 0.21875)
    later_conv_bias = scatter_about(splits[8], (OCH,), 0.5, 3.0, (), jnp.float32)
    shortcut_weight = scatter_about(splits[9], (OCH, CIN), CIN ** -0.5, 0.5)
    return {"global_field": global_field, "regional_state": regional_state, "windows": windows, "longitude_weights": longitude_weights, "latitude_weights": latitude_weights, "first_kernel": first_kernel, "first_bias": first_bias, "second_kernel": second_kernel, "later_conv_bias": later_conv_bias, "shortcut_weight": shortcut_weight}


def domain_field(tiles, domain):
    per_domain = N_TILE // 2
    tile_rows_count = per_domain // TCOLS
    block = tiles[domain * per_domain:(domain + 1) * per_domain]
    channels = block.shape[1]
    block = block.reshape(tile_rows_count, TCOLS, channels, HY, HX).transpose(2, 0, 3, 1, 4)
    return block.reshape(channels, tile_rows_count * HY, TCOLS * HX)


def field_tiles(field):
    per_domain = N_TILE // 2
    tile_rows_count = per_domain // TCOLS
    channels = field.shape[0]
    block = field.reshape(channels, tile_rows_count, HY, TCOLS, HX).transpose(1, 3, 0, 2, 4)
    return block.reshape(per_domain, channels, HY, HX)


def convolve(padded, kernel, out_rows, out_cols):
    total = jnp.zeros((kernel.shape[2], out_rows, out_cols), jnp.float32)
    for vertical in range(3):
        for lateral in range(3):
            window = padded[:, vertical:vertical + out_rows, lateral:lateral + out_cols].astype(jnp.float32)
            total = total + jnp.einsum("oc,chw->ohw", kernel[vertical, lateral].astype(jnp.float32), window)
    return total


def reference(global_field, regional_state, windows, longitude_weights, latitude_weights, first_kernel, first_bias, second_kernel, later_conv_bias, shortcut_weight):
    rotation = N_TILE // 4 + 2
    groups = []
    for group in range(N_REGION):
        groups.append(jnp.roll(regional_state[group * N_TILE:(group + 1) * N_TILE], rotation, axis=0))
    arranged = jnp.concatenate(groups, axis=0)
    results = []
    for domain in range(DOMAINS):
        lat_start = windows[domain, 0]
        lat_count = windows[domain, 1]
        lon_start = windows[domain, 2]
        lon_count = windows[domain, 3]
        longitude_matrix = longitude_weights[domain].astype(jnp.float32) * (jnp.arange(KWIN) < lon_count).astype(jnp.float32)[None, :]
        lat_mat = latitude_weights[domain].astype(jnp.float32) * (jnp.arange(LWIN) < lat_count).astype(jnp.float32)[None, :]
        incoming_field = lax.dynamic_slice_in_dim(global_field, lon_start, KWIN, 2).astype(jnp.float32)
        latitude_strips = jnp.einsum("yep,bp->yeb", incoming_field, longitude_matrix).astype(jnp.bfloat16)
        picked = lax.dynamic_slice_in_dim(latitude_strips, lat_start, LWIN, 1).astype(jnp.float32)
        condition = jnp.einsum("yl,clx->cyx", lat_mat, picked).astype(jnp.bfloat16)
        inputs = jnp.concatenate([domain_field(arranged, domain), condition], axis=0)
        total_row_count = inputs.shape[1]
        cols_total = inputs.shape[2]
        padded = jnp.pad(inputs, ((0, 0), (1, 1), (1, 1)))
        first = convolve(padded, first_kernel, total_row_count, cols_total) + first_bias[:, None, None]
        hidden = jax.nn.silu(first).astype(jnp.bfloat16)
        padded_hidden = jnp.pad(hidden, ((0, 0), (1, 1), (1, 1)))
        second = convolve(padded_hidden, second_kernel, total_row_count, cols_total) + later_conv_bias[:, None, None]
        skipped = jnp.einsum("oc,chw->ohw", shortcut_weight.astype(jnp.float32), inputs.astype(jnp.float32))
        output = (second + skipped).astype(jnp.bfloat16)
        results.append(field_tiles(output))
    placed = jnp.concatenate(results, axis=0)
    outputs = []
    for group in range(N_REGION):
        outputs.append(jnp.roll(placed[group * N_TILE:(group + 1) * N_TILE], -rotation, axis=0))
    return jnp.concatenate(outputs, axis=0)
```

```python
import jax
import jax.numpy as jnp
import numpy as np
from jax import lax
from jax.sharding import PartitionSpec as P

TCOLS = 4
ROWS = 8
EVERY = ("region", "tile")


def domain_half(tile, tiles, rotation):
    return ((tile + rotation) % tiles) // (tiles // 2)


def routes(regions, tiles, rotation):
    bands = tiles // ROWS
    half = [[domain_half(ROWS * k + g, tiles, rotation) for k in range(bands)] for g in range(ROWS)]
    by_row, by_domain, rows = [], [], np.zeros((tiles, 2), np.int32)
    for z in range(regions):
        for g in range(ROWS):
            by_row.append([z * tiles + k * ROWS + g for k in range(bands)])
    for g in range(ROWS):
        lower = [k for k in range(bands) if half[g][k] == 0]
        upper = [k for k in range(bands) if half[g][k] == 1]
        for pair in zip(lower, upper):
            by_domain.append([z * tiles + k * ROWS + g for z in range(regions) for k in pair])
            for k in pair:
                rows[k * ROWS + g] = [ROWS * g + pair[0], ROWS * g + pair[1]]
    tile_half = [domain_half(t, tiles, rotation) for t in range(tiles)]
    spread, table = [], np.zeros((2, 2, tiles), np.int32)
    for z in range(regions):
        for h in range(2):
            for core in range(2):
                spread.append([z * tiles + t for t in range(tiles) if tile_half[t] == h and t % 2 == core])
    for h in range(2):
        for core in range(2):
            mine = [t for t in range(tiles) if tile_half[t] == h and t % 2 == core]
            other = [t for t in range(tiles) if tile_half[t] == h and t % 2 != core]
            table[h, core] = np.concatenate([rows[t] for t in mine + other])
    return by_row, by_domain, spread, table


def swap(value, groups):
    return lax.all_to_all(
        value, EVERY, split_axis=0, concat_axis=0, axis_index_groups=groups, tiled=True
    )


def from_neighbour(block, distance):
    size = lax.axis_size("tile")
    return lax.ppermute(block, "tile", [((i - distance) % size, i) for i in range(size)])


def window_rows(global_field, windows, region_index, tile_index, tile_count, rotation):
    regions = lax.axis_size("region")
    by_row, by_domain, spread, table = routes(regions, tile_count, rotation)
    lon = global_field.shape[2]
    bands = tile_count // ROWS
    width = 128
    band, lane = tile_index // ROWS, tile_index % ROWS
    by_rows = swap(global_field.transpose(1, 0, 2), by_row)
    lat_start, lon_start = windows[:, 0], windows[:, 2]
    residue = ROWS * lane + band
    source = (lat_start + (residue - lat_start) % 64) // 64
    offset = lon_start - lon * region_index
    chooser = (
        lax.broadcasted_iota(jnp.int32, (8, lon, width), 1)
        == lax.broadcasted_iota(jnp.int32, (8, lon, width), 2) + offset[:, None, None]
    ).astype(jnp.bfloat16)
    chosen = jnp.stack(
        [lax.dynamic_index_in_dim(by_rows, source[d], 0, keepdims=False) for d in range(8)]
    )
    parts = jnp.einsum("dck,dkn->dcn", chosen, chooser, preferred_element_type=jnp.float32)
    parts = jnp.pad(parts.astype(jnp.bfloat16), ((0, 0), (0, 2), (0, 0)))
    mixed = swap(parts, by_domain)
    piece = mixed.reshape(regions, 2, *parts.shape[1:]).astype(jnp.float32).sum(0)
    piece = piece.astype(jnp.bfloat16)
    sharers = len(spread[0])
    mine = swap(jnp.broadcast_to(piece[None], (sharers, *piece.shape)), spread)
    pairs = [(i, i ^ 1) for i in range(regions * tile_count)]
    other = lax.ppermute(mine, EVERY, pairs)
    whole = jnp.concatenate([mine, other], axis=0)
    whole = whole.reshape(-1, *whole.shape[2:])
    return whole, table


def shards(
    global_field,
    regional_state,
    windows,
    longitude_weights,
    latitude_weights,
    first_kernel,
    first_bias,
    second_kernel,
    later_conv_bias,
    shortcut_weight,
):
    tile_count = lax.axis_size("tile")
    tile_index = lax.axis_index("tile")
    region_index = lax.axis_index("region")
    half_count = tile_count // 2
    row_tiles = half_count // TCOLS
    rotation = tile_count // 4 + 2
    position = (tile_index + rotation) % tile_count
    half = position // half_count
    within = position % half_count
    row_tile, col_tile = within // TCOLS, within % TCOLS
    my_domain = 2 * region_index + half
    tile_rows, tile_cols = regional_state.shape[2:]
    top, bottom = row_tile > 0, row_tile < row_tiles - 1
    left, right = col_tile > 0, col_tile < TCOLS - 1

    whole, table = window_rows(
        global_field, windows, region_index, tile_index, tile_count, rotation
    )
    own = lax.dynamic_index_in_dim(windows, my_domain, 0, keepdims=False)
    rho = lax.dynamic_slice(jnp.asarray(table), (half, tile_index % 2, 0), (1, 1, 64))[0, 0]
    order = (rho - own[0]) % 64
    lat = lax.dynamic_index_in_dim(latitude_weights, half, 0, keepdims=False)
    lat = jnp.pad(lat, ((2, 2), (0, 0)))
    lat = lax.dynamic_slice_in_dim(lat, row_tile * tile_rows, tile_rows + 4, 0)
    picks = (lax.broadcasted_iota(jnp.int32, (64, 64), 0) == order[None, :]) & (
        order[None, :] < own[1]
    )
    lat = jnp.dot(lat, picks.astype(jnp.bfloat16), preferred_element_type=jnp.float32)
    lat = lat.astype(jnp.bfloat16)
    lon = lax.dynamic_index_in_dim(longitude_weights, my_domain, 0, keepdims=False)
    lon = lon * (jnp.arange(128) < own[3]).astype(jnp.bfloat16)[None, :]
    lon = jnp.pad(lon, ((2, 2), (0, 0)))
    lon = lax.dynamic_slice_in_dim(lon, col_tile * tile_cols, tile_cols + 4, 0)

    state = regional_state[0]
    above = from_neighbour(state[:, tile_rows - 2 :, :], TCOLS) * top.astype(state.dtype)
    below = from_neighbour(state[:, :2, :], -TCOLS) * bottom.astype(state.dtype)
    tall = jnp.concatenate([above, state, below], axis=1)
    west = from_neighbour(tall[:, :, tile_cols - 2 :].transpose(2, 0, 1), 1)
    east = from_neighbour(tall[:, :, :2].transpose(2, 0, 1), -1)
    west = (west * left.astype(state.dtype)).transpose(1, 2, 0)
    east = (east * right.astype(state.dtype)).transpose(1, 2, 0)
    wide = jnp.concatenate([west, tall, east], axis=2)

    strips = jnp.einsum("sck,xk->scx", whole, lon, preferred_element_type=jnp.float32)
    strips = strips.astype(jnp.bfloat16)
    condition = jnp.einsum("ys,scx->cyx", lat, strips, preferred_element_type=jnp.float32)
    condition = condition[:70].astype(jnp.bfloat16)
    inputs = jnp.concatenate([wide, condition], axis=0)
    dims = ("NCHW", "HWOI", "NCHW")
    first = lax.conv_general_dilated(
        inputs[None], first_kernel, (1, 1), "VALID", dimension_numbers=dims,
        preferred_element_type=jnp.float32,
    )[0] + first_bias[:, None, None]
    hidden = jax.nn.silu(first).astype(jnp.bfloat16)
    y = jnp.arange(tile_rows + 2)
    x = jnp.arange(tile_cols + 2)
    keep_y = ((y > 0) | top) & ((y <= tile_rows) | bottom)
    keep_x = ((x > 0) | left) & ((x <= tile_cols) | right)
    hidden = jnp.where(keep_y[None, :, None] & keep_x[None, None, :], hidden, 0)
    second = lax.conv_general_dilated(
        hidden[None], second_kernel, (1, 1), "VALID", dimension_numbers=dims,
        preferred_element_type=jnp.float32,
    )[0] + later_conv_bias[:, None, None]
    centre = inputs[:, 2 : 2 + tile_rows, 2 : 2 + tile_cols]
    skipped = jnp.einsum("oc,chw->ohw", shortcut_weight, centre, preferred_element_type=jnp.float32)
    return (second + skipped)[None].astype(jnp.bfloat16)


def solution(mesh):
    placed = (
        P(None, "tile", "region"),
        P(("region", "tile"), None, None, None),
        P(),
        P(),
        P("region", None, None),
        P(),
        P(),
        P(),
        P(),
        P(),
    )
    return jax.shard_map(
        shards,
        mesh=mesh,
        in_specs=placed,
        out_specs=P(("region", "tile"), None, None, None),
        check_vma=False,
    )
```

```python
import jax
import jax.numpy as jnp
import numpy as np
from jax import lax
from jax.experimental import pallas as pl
from jax.experimental.pallas import tpu as pltpu
from jax.sharding import PartitionSpec as P

TCOLS = 4
ROWS = 8
EVERY = ("region", "tile")
SP = 112
CP = 80
WP = 72
YP = 72


def taps(kernel, lo, hi, pad, order):
    part = jnp.pad(kernel[:, :, :, lo:hi], ((0, 0), (0, 0), (0, 0), (0, pad - (hi - lo))))
    part = part.transpose(order)
    return part.reshape(part.shape[0] * part.shape[1], part.shape[2] * pad)


def edge_taps(kernel, lo, hi, pad, q):
    part = jnp.pad(kernel[:, q, :, lo:hi], ((0, 0), (0, 0), (0, pad - (hi - lo))))
    return part.reshape(-1, pad)


def pack_weights(first_kernel, second_kernel, shortcut, sch):
    cin = first_kernel.shape[3]
    main, side = (1, 2, 0, 3), (0, 2, 1, 3)
    def with_skip(matrix, lo, hi, pad):
        skip = jnp.pad(shortcut[:, lo:hi], ((0, 0), (pad, 2 * pad - (hi - lo))))
        return jnp.concatenate([matrix, skip], axis=0)
    return (
        with_skip(taps(first_kernel, 0, sch, SP, main), 0, sch, SP),
        with_skip(taps(first_kernel, sch, cin, CP, main), sch, cin, CP),
        taps(first_kernel, 0, sch, SP, side),
        taps(first_kernel, sch, cin, CP, side),
        jnp.stack([edge_taps(first_kernel, 0, sch, SP, q) for q in (0, 2)]),
        jnp.stack([edge_taps(first_kernel, sch, cin, CP, q) for q in (0, 2)]),
        taps(second_kernel, 0, second_kernel.shape[3], second_kernel.shape[3], main),
        jnp.stack([edge_taps(second_kernel, 0, 96, 96, q) for q in (0, 2)]),
    )


def mm(a, b):
    return jnp.dot(a, b, preferred_element_type=jnp.float32)


def body(
    flags, xs, ps, wa, wb, lont, lat, latt, w1s, w1c, v1s, v1c, e1s, e1c, w2, e2w, b1, b2,
    out, bands, sideb, cf, ch, cs, pc, hid, skip, edge1, edge2, of,
):
    f32, bf16 = jnp.float32, jnp.bfloat16
    och = b1.shape[0]
    half = wa.shape[0]
    step = 288

    def spread(k, _):
        at = pl.multiple_of(k * step, 16)
        for base, part in ((0, wa), (half, wb)):
            got = mm(part[pl.ds(at, step), :], lont[...])
            to = pl.ds(pl.multiple_of(base + at, 16), step)
            bands[to, :] = got[:, :128]
            sideb[to, :] = got[:, 128:]
        return 0

    lax.fori_loop(0, half // step, spread, 0)

    lane = lax.broadcasted_iota(jnp.int32, (64, 128), 1)

    def rows(k, _):
        pair = [
            bands[pl.ds(2 * k + m, 64, stride=WP), :].astype(bf16) for m in range(2)
        ]
        got = mm(lat[...], jnp.concatenate(pair, axis=1))
        cf[pl.ds(pl.multiple_of(2 * k * YP, 8), YP), :] = got[:, :128]
        cf[pl.ds(pl.multiple_of((2 * k + 1) * YP, 8), YP), :] = got[:, 128:]
        return 0

    lax.fori_loop(0, WP // 2, rows, 0, unroll=4)

    for b in range(CP // 16):
        packed = jnp.zeros((64, 128), f32)
        for c in range(min(16, WP - 16 * b)):
            one = sideb[pl.ds(16 * b + c, 64, stride=WP), :]
            packed = jnp.where(lane // 8 == c, one, packed)
        ch[pl.ds(128 * b, 128), :] = mm(packed.T.astype(bf16), latt[...])
    for x in range(6):
        side, k = x // 3, x % 3
        for b in range(CP // 16):
            pc[pl.ds(CP * k + 16 * b, 16), pl.ds(128 * side, 128)] = ch[
                pl.ds(128 * b + x, 16, stride=8), :
            ].astype(bf16)

    def turn(y, _):
        one = cf[pl.ds(y, WP, stride=YP), :]
        one = jnp.concatenate([one, jnp.zeros((CP - WP, 128), f32)], axis=0)
        cs[pl.ds(pl.multiple_of(CP * y, 16), CP), :] = one.astype(bf16)
        return 0

    lax.fori_loop(0, 68, turn, 0, unroll=4)

    def along(parts):
        return (
            parts[:och]
            + pltpu.roll(parts[och : 2 * och], 127, 1)
            + pltpu.roll(parts[2 * och :], 126, 1)
        )

    lane1 = lax.broadcasted_iota(jnp.int32, (och, 128), 1)
    got = mm(v1s[...], ps[...]) + mm(v1c[...], pc[...])
    for side in range(2):
        at = pl.ds(128 * side, 128)
        v = along(got[:, 128 * side : 128 * side + 128]) + b1[...]
        v = v / (1.0 + jnp.exp(-v))
        keep = (
            ((lane1 > 0) | (flags[0] > 0))
            & ((lane1 < 65) | (flags[1] > 0))
            & (lane1 < 66)
            & (flags[2 + side] > 0)
        )
        v = jnp.where(keep, v, 0.0).astype(bf16)
        edge2[side] = along(mm(e2w[side], v))
        edge1[side] = along(
            mm(e1s[side], ps[pl.ds(SP, SP), at]) + mm(e1c[side], pc[pl.ds(CP, CP), at])
        )

    first_lane, last_lane = lane1 == 0, lane1 == 127

    def across(parts, edges, at):
        west = jnp.where(first_lane, pltpu.roll(edges[0], 128 - at, 1), pltpu.roll(parts[:och], 1, 1))
        east = jnp.where(
            last_lane, pltpu.roll(edges[1], 127 - at, 1), pltpu.roll(parts[2 * och : 3 * och], 127, 1)
        )
        return parts[och : 2 * och] + west + east

    def conv1(i, _):
        r = 2 * i
        state = [xs[pl.ds(pl.multiple_of(SP * (r + m), 16), 3 * SP), :] for m in range(2)]
        cond = [cs[pl.ds(pl.multiple_of(CP * (r + m), 16), 3 * CP), :] for m in range(2)]
        got = mm(w1s[...], jnp.concatenate(state, axis=1)) + mm(
            w1c[...], jnp.concatenate(cond, axis=1)
        )
        for m in range(2):
            parts = got[:, 128 * m : 128 * m + 128]
            v = across(parts, edge1, r + m) + b1[...]
            v = v / (1.0 + jnp.exp(-v))
            live = jnp.where(
                r + m == 0, flags[0], jnp.where(r + m == 65, flags[1], 1)
            ).astype(f32)
            hid[pl.ds(pl.multiple_of(och * (r + m), 16), och), :] = (v * live).astype(bf16)
            skip[pl.ds(pl.multiple_of(och * (r + m), 8), och), :] = parts[3 * och :]
        return 0

    lax.fori_loop(0, 33, conv1, 0)

    def conv2(j, _):
        y = 2 * j
        rows = [hid[pl.ds(pl.multiple_of(och * (y + m), 16), 3 * och), :] for m in range(2)]
        got = mm(w2[...], jnp.concatenate(rows, axis=1))
        for m in range(2):
            v = across(got[:, 128 * m : 128 * m + 128], edge2, y + m)
            v = v + skip[pl.ds(pl.multiple_of(och * (y + m + 1), 8), och), :] + b2[...]
            of[pl.ds(y + m, och, stride=YP), :] = v
        return 0

    lax.fori_loop(0, 32, conv2, 0)

    def leave(o, _):
        out[o] = of[pl.ds(pl.multiple_of(YP * o, 8), 64), :].astype(bf16)
        return 0

    lax.fori_loop(0, och, leave, 0, unroll=4)


def block(flags, xs, ps, wa, wb, lont, lat, latt, weights, b1, b2, interpret=False):
    f32, bf16 = jnp.float32, jnp.bfloat16
    och = b1.shape[0]
    vm = lambda shape, t: pltpu.VMEM(shape, t)
    spec = pl.BlockSpec(memory_space=pltpu.VMEM)
    return pl.pallas_call(
        body,
        out_shape=jax.ShapeDtypeStruct((och, 64, 128), bf16),
        in_specs=[pl.BlockSpec(memory_space=pltpu.SMEM)] + [spec] * 17,
        out_specs=spec,
        scratch_shapes=[
            vm((64 * WP, 128), f32),
            vm((64 * WP, 128), f32),
            vm((WP * YP, 128), f32),
            vm((128 * CP // 16, 128), f32),
            vm((68 * CP, 128), bf16),
            vm((3 * CP, 256), bf16),
            vm((66 * och, 128), bf16),
            vm((66 * och, 128), f32),
            vm((2, och, 128), f32),
            vm((2, och, 128), f32),
            vm((och * YP, 128), f32),
        ],
        compiler_params=pltpu.CompilerParams(vmem_limit_bytes=44 * 2**20),
        cost_estimate=pl.CostEstimate(flops=8 * 10**9, bytes_accessed=8 * 2**20, transcendentals=10**6),
        interpret=interpret,
        name="block",
    )(flags, xs, ps, wa, wb, lont, lat, latt, *weights, b1[:, None], b2[:, None])


def lon_matrix(lon):
    six = jnp.concatenate([lon[:3], lon[129:132], jnp.zeros((2, 128), lon.dtype)], axis=0)
    return jnp.concatenate([lon[2:130], jnp.tile(six, (16, 1))], axis=0).T


def lat_matrices(lat):
    full = jnp.pad(lat, ((0, 60), (0, 0)))
    return full[:YP], full.T


def domain_half(tile, tiles, rotation):
    return ((tile + rotation) % tiles) // (tiles // 2)


def routes(regions, tiles, rotation):
    bands = tiles // ROWS
    half = [[domain_half(ROWS * k + g, tiles, rotation) for k in range(bands)] for g in range(ROWS)]
    by_row, by_domain, rows = [], [], np.zeros((tiles, 2), np.int32)
    for z in range(regions):
        for g in range(ROWS):
            by_row.append([z * tiles + k * ROWS + g for k in range(bands)])
    for g in range(ROWS):
        lower = [k for k in range(bands) if half[g][k] == 0]
        upper = [k for k in range(bands) if half[g][k] == 1]
        for pair in zip(lower, upper):
            by_domain.append([z * tiles + k * ROWS + g for z in range(regions) for k in pair])
            for k in pair:
                rows[k * ROWS + g] = [ROWS * g + pair[0], ROWS * g + pair[1]]
    tile_half = [domain_half(t, tiles, rotation) for t in range(tiles)]
    spread, table = [], np.zeros((2, 2, tiles), np.int32)
    for z in range(regions):
        for h in range(2):
            for core in range(2):
                spread.append([z * tiles + t for t in range(tiles) if tile_half[t] == h and t % 2 == core])
    for h in range(2):
        for core in range(2):
            mine = [t for t in range(tiles) if tile_half[t] == h and t % 2 == core]
            other = [t for t in range(tiles) if tile_half[t] == h and t % 2 != core]
            table[h, core] = np.concatenate([rows[t] for t in mine + other])
    return by_row, by_domain, spread, table


def swap(value, groups):
    return lax.all_to_all(
        value, EVERY, split_axis=0, concat_axis=0, axis_index_groups=groups, tiled=True
    )


def from_neighbour(block, distance):
    size = lax.axis_size("tile")
    return lax.ppermute(block, "tile", [((i - distance) % size, i) for i in range(size)])


def window_rows(global_field, windows, region_index, tile_index, tile_count, rotation):
    regions = lax.axis_size("region")
    by_row, by_domain, spread, table = routes(regions, tile_count, rotation)
    lon = global_field.shape[2]
    bands = tile_count // ROWS
    width = 128
    band, lane = tile_index // ROWS, tile_index % ROWS
    by_rows = swap(global_field.transpose(1, 0, 2), by_row)
    lat_start, lon_start = windows[:, 0], windows[:, 2]
    residue = ROWS * lane + band
    source = (lat_start + (residue - lat_start) % 64) // 64
    offset = lon_start - lon * region_index
    chooser = (
        lax.broadcasted_iota(jnp.int32, (8, lon, width), 1)
        == lax.broadcasted_iota(jnp.int32, (8, lon, width), 2) + offset[:, None, None]
    ).astype(jnp.bfloat16)
    chosen = jnp.stack(
        [lax.dynamic_index_in_dim(by_rows, source[d], 0, keepdims=False) for d in range(8)]
    )
    parts = jnp.einsum("dck,dkn->dcn", chosen, chooser, preferred_element_type=jnp.float32)
    parts = jnp.pad(parts.astype(jnp.bfloat16), ((0, 0), (0, 2), (0, 0)))
    mixed = swap(parts, by_domain)
    piece = mixed.reshape(regions, 2, *parts.shape[1:]).astype(jnp.float32).sum(0)
    piece = piece.astype(jnp.bfloat16)
    return piece, spread, table


def spread_pieces(piece, spread, ready):
    piece, ready = lax.optimization_barrier((piece, ready))
    sharers = len(spread[0])
    mine = swap(jnp.broadcast_to(piece[None], (sharers, *piece.shape)), spread)
    mine = mine.reshape(-1, piece.shape[-1])
    devices = lax.axis_size("region") * lax.axis_size("tile")
    other = lax.ppermute(mine, EVERY, [(i, i ^ 1) for i in range(devices)])
    return mine, other, ready


def shards(
    global_field,
    regional_state,
    windows,
    longitude_weights,
    latitude_weights,
    first_kernel,
    first_bias,
    second_kernel,
    later_conv_bias,
    shortcut_weight,
):
    tile_count = lax.axis_size("tile")
    tile_index = lax.axis_index("tile")
    region_index = lax.axis_index("region")
    half_count = tile_count // 2
    row_tiles = half_count // TCOLS
    rotation = tile_count // 4 + 2
    position = (tile_index + rotation) % tile_count
    half = position // half_count
    within = position % half_count
    row_tile, col_tile = within // TCOLS, within % TCOLS
    my_domain = 2 * region_index + half
    tile_rows, tile_cols = regional_state.shape[2:]
    top, bottom = row_tile > 0, row_tile < row_tiles - 1
    left, right = col_tile > 0, col_tile < TCOLS - 1

    piece, spread, table = window_rows(
        global_field, windows, region_index, tile_index, tile_count, rotation
    )
    own = lax.dynamic_index_in_dim(windows, my_domain, 0, keepdims=False)
    rho = lax.dynamic_slice(jnp.asarray(table), (half, tile_index % 2, 0), (1, 1, 64))[0, 0]
    order = (rho - own[0]) % 64
    lat = lax.dynamic_index_in_dim(latitude_weights, half, 0, keepdims=False)
    lat = jnp.pad(lat, ((2, 2), (0, 0)))
    lat = lax.dynamic_slice_in_dim(lat, row_tile * tile_rows, tile_rows + 4, 0)
    picks = (lax.broadcasted_iota(jnp.int32, (64, 64), 0) == order[None, :]) & (
        order[None, :] < own[1]
    )
    lat = jnp.dot(lat, picks.astype(jnp.bfloat16), preferred_element_type=jnp.float32)
    lat = lat.astype(jnp.bfloat16)
    lon = lax.dynamic_index_in_dim(longitude_weights, my_domain, 0, keepdims=False)
    lon = lon * (jnp.arange(128) < own[3]).astype(jnp.bfloat16)[None, :]
    lon = jnp.pad(lon, ((2, 2), (0, 0)))
    lon = lax.dynamic_slice_in_dim(lon, col_tile * tile_cols, tile_cols + 4, 0)

    state = regional_state[0]
    above = from_neighbour(state[:, tile_rows - 2 :, :], TCOLS) * top.astype(state.dtype)
    below = from_neighbour(state[:, :2, :], -TCOLS) * bottom.astype(state.dtype)
    tall = jnp.concatenate([above, state, below], axis=1)
    first_cols = tall[:, :, :2].transpose(2, 0, 1)
    last_cols = tall[:, :, tile_cols - 2 :].transpose(2, 0, 1)
    west = from_neighbour(last_cols, 1) * left.astype(state.dtype)
    east = from_neighbour(first_cols, -1) * right.astype(state.dtype)
    channels = state.shape[0]
    xs = jnp.pad(tall.transpose(1, 0, 2), ((0, 0), (0, SP - channels), (0, 0)))
    xs = xs.reshape(-1, tile_cols)
    sides = [
        jnp.concatenate([west, first_cols[:1]], axis=0),
        jnp.concatenate([last_cols[1:], east], axis=0),
    ]
    sides = [jnp.pad(s, ((0, 0), (0, SP - channels), (0, 60))) for s in sides]
    ps = jnp.concatenate(sides, axis=2).reshape(3 * SP, 256)
    weights = pack_weights(first_kernel, second_kernel, shortcut_weight, channels)
    lat, latt = lat_matrices(lat)
    flags = jnp.stack([top, bottom, left, right]).astype(jnp.int32)
    lont = lon_matrix(lon)
    ready = (xs, ps, weights, lat, latt, lont, flags)
    mine, other, ready = spread_pieces(piece, spread, ready)
    xs, ps, weights, lat, latt, lont, flags = ready
    out = block(
        flags, xs, ps, mine, other, lont, lat, latt, weights, first_bias, later_conv_bias
    )
    return out[None]


def solution(mesh):
    placed = (
        P(None, "tile", "region"),
        P(("region", "tile"), None, None, None),
        P(),
        P(),
        P("region", None, None),
        P(),
        P(),
        P(),
        P(),
        P(),
    )
    return jax.shard_map(
        shards,
        mesh=mesh,
        in_specs=placed,
        out_specs=P(("region", "tile"), None, None, None),
        check_vma=False,
    )
```

```python
import jax
import jax.numpy as jnp
import numpy as np
from jax import lax
from jax.experimental import pallas as pl
from jax.experimental.pallas import tpu as pltpu
from jax.sharding import PartitionSpec as P


TCOLS = 4
ROWS = 8
EVERY = ("region", "tile")
SP = 112
CP = 80
WP = 72
YP = 72
F32, BF16 = jnp.float32, jnp.bfloat16


def mm(a, b):
    return jnp.dot(a, b, preferred_element_type=F32)


def mm_t(a, b):
    return lax.dot_general(a, b, (((1,), (1,)), ((), ())), preferred_element_type=F32)


def iota(shape, dim):
    return lax.broadcasted_iota(jnp.int32, shape, dim)


def chosen(cond):
    return jnp.where(cond, 1.0, 0.0).astype(BF16)


def column(row):
    n = row.shape[1]
    hit = iota((n, n), 0) == iota((n, n), 1)
    return jnp.sum(jnp.where(hit, row, 0.0), axis=1, keepdims=True)


def rows_at(start, size, unit):
    return pl.ds(pl.multiple_of(start, unit), size)


def along(parts, och):
    return (
        parts[:och]
        + pltpu.roll(parts[och : 2 * och], 127, 1)
        + pltpu.roll(parts[2 * och : 3 * och], 126, 1)
    )


def across(parts, edges, at, och):
    lane = iota((och, 128), 1)
    west = jnp.where(lane == 0, pltpu.roll(edges[0], 128 - at, 1), pltpu.roll(parts[:och], 1, 1))
    east = jnp.where(
        lane == 127, pltpu.roll(edges[1], 127 - at, 1), pltpu.roll(parts[2 * och : 3 * och], 127, 1)
    )
    return parts[och : 2 * och] + west + east


def stacked(k3, q, och):
    return jnp.concatenate([k3[p, q * och : (q + 1) * och, :] for p in range(3)], axis=0)


def turn_body(state, xs, strips, flat, packs):
    chans, height = state.shape[0], state.shape[1]

    def widen(c, _):
        flat[rows_at(YP * c, height, 8), :] = state[c].astype(F32)
        return 0

    lax.fori_loop(0, chans, widen, 0, unroll=3)
    flat[pl.ds(YP * chans, YP * (SP - chans)), :] = jnp.zeros((YP * (SP - chans), 128), F32)

    def row(y, _):
        xs[rows_at(SP * y, SP, 16), :] = flat[pl.ds(y, SP, stride=YP), :].astype(BF16)
        return 0

    lax.fori_loop(0, height, row, 0, unroll=4)
    lane = iota((height, 128), 1)
    for b in range(4):
        packed = jnp.zeros((height, 128), F32)
        for c in range(min(32, chans - 32 * b)):
            one = pltpu.roll(flat[pl.ds(YP * (32 * b + c), height), :], (2 + 4 * c) % 128, 1)
            packed = jnp.where(lane // 4 == c, one, packed)
        packed = jnp.concatenate([packed, jnp.zeros((128 - height, 128), F32)], axis=0)
        packs[pl.ds(128 * b, 128), :] = packed.T
    for col in range(4):
        for b in range(4):
            n = min(32, SP - 32 * b)
            strips[pl.ds(SP * col + 32 * b, n), :] = packs[
                pl.ds(128 * b + col, n, stride=4), :
            ].astype(BF16)


def corner_body(scal, strips, above, below, ext):
    lane = iota((SP, 128), 1)
    top, bottom = scal[0] > 0, scal[1] > 0
    for j, x in enumerate((126, 127, 0, 1)):
        e = pltpu.roll(strips[pl.ds(SP * j, SP), :].astype(F32), 2, 1)
        for m in range(2):
            up = pltpu.roll(above[pl.ds(SP * m, SP), :].astype(F32), (m - x) % 128, 1)
            down = pltpu.roll(below[pl.ds(SP * m, SP), :].astype(F32), (66 + m - x) % 128, 1)
            e = jnp.where((lane == m) & top, up, e)
            e = jnp.where((lane == 66 + m) & bottom, down, e)
        ext[pl.ds(SP * j, SP), :] = e.astype(BF16)


def early_body(
    scal, xs_own, above, below, ext, west, east, k1, sw, k2, lon, lat, rho, b1, b2,
    acc, skip, side, w1c, v1c, e1c, w2, lonb, latb,
    xs, w1s, sem,
):
    och = sw.shape[0]
    cin = sw.shape[1]
    sch = cin - 70
    fetch = pltpu.make_async_copy(xs_own, xs.at[pl.ds(2 * SP, 64 * SP)], sem)
    fetch.start()
    top, bottom, left, right = scal[0] > 0, scal[1] > 0, scal[2] > 0, scal[3] > 0
    xs[pl.ds(0, 2 * SP), :] = jnp.where(top, above[...], 0)
    xs[pl.ds(66 * SP, 2 * SP), :] = jnp.where(bottom, below[...], 0)
    bias1, bias2 = column(b1[...]), column(b2[...])

    row_s, col_s = iota((cin, 3 * SP), 0), iota((cin, 3 * SP), 1)
    row_c, col_c = iota((cin, 3 * CP), 0), iota((cin, 3 * CP), 1)
    put_s = [chosen((col_s == SP * p + row_s) & (row_s < sch)) for p in range(3)]
    put_c = [chosen((col_c == CP * p + row_c - sch) & (row_c >= sch)) for p in range(3)]
    w1s[pl.ds(0, 3 * och), :] = sum(mm(k1[p], put_s[p]) for p in range(3)).astype(BF16)
    w1s[pl.ds(3 * och, och), :] = mm(sw[...], put_s[1]).astype(BF16)
    w1c[pl.ds(0, 3 * och), :] = sum(mm(k1[p], put_c[p]) for p in range(3)).astype(BF16)
    w1c[pl.ds(3 * och, och), :] = mm(sw[...], put_c[1]).astype(BF16)
    turned = [stacked(k1, q, och) for q in range(3)]
    v1s = sum(mm(turned[q], put_s[q]) for q in range(3)).astype(BF16)
    v1c[...] = sum(mm(turned[q], put_c[q]) for q in range(3)).astype(BF16)
    row_e, col_e = iota((cin, CP), 0), iota((cin, CP), 1)
    put_e = chosen((col_e == row_e - sch) & (row_e >= sch))
    e1c[0] = mm(turned[0], put_e).astype(BF16)
    e1c[1] = mm(turned[2], put_e).astype(BF16)
    row_2, col_2 = iota((och, 3 * och), 0), iota((och, 3 * och), 1)
    w2[...] = sum(mm(k2[p], chosen(col_2 == och * p + row_2)) for p in range(3)).astype(BF16)

    masked = jnp.where(iota((512, 128), 1) < scal[8], lon[0], 0)
    r, c = iota((256, 512), 0), iota((256, 512), 1)
    six = (r - 128) % 8
    off = jnp.where(r < 128, r, jnp.where(six < 3, six - 2, six + 124))
    pick = chosen((c == off + 128 * scal[5]) & ((r < 128) | (six < 6)))
    lonb[...] = mm(pick, masked).astype(BF16)
    r, c = iota((128, 512), 0), iota((128, 512), 1)
    pick = chosen((c == r - 2 + 64 * scal[4]) & (r < 68))
    taken = mm(pick, lat[0]).astype(BF16)
    want = (rho[...] - scal[6]) & 63
    order = chosen((iota((64, 64), 0) == want) & (want < scal[7]))
    latb[...] = mm(taken, order).astype(BF16)

    west_in = jnp.where(left, west[...], 0)
    east_in = jnp.where(right, east[...], 0)
    ps = jnp.concatenate(
        [
            jnp.concatenate([west_in, ext[pl.ds(2 * SP, SP), :]], axis=0),
            jnp.concatenate([ext[pl.ds(SP, SP), :], east_in], axis=0),
        ],
        axis=1,
    )
    got = mm(v1s, ps)
    for s in range(2):
        side[:, 128 * s : 128 * s + 128] = along(got[:, 128 * s : 128 * s + 128], och) + bias1
    edges = [
        along(mm(turned[0][:, :SP], west_in[SP:]), och),
        along(mm(turned[2][:, :SP], east_in[:SP]), och),
    ]
    fetch.wait()

    def conv(i, _):
        rows = [xs[rows_at(SP * (2 * i + m), 3 * SP, 16), :] for m in range(2)]
        got = mm(w1s[...], jnp.concatenate(rows, axis=1))
        for m in range(2):
            parts = got[:, 128 * m : 128 * m + 128]
            at = rows_at(och * (2 * i + m), och, 16)
            acc[at, :] = across(parts, edges, 2 * i + m, och) + bias1
            skip[at, :] = parts[3 * och :] + bias2
        return 0

    lax.fori_loop(0, 33, conv, 0)


def late_body(
    scal, wa, wb, lonb, latb, w1c, v1c, e1c, w2, k2, side, acc_hbm, skip_hbm,
    out, bands, sideb, cf, ch, cs, pc, hid, acc, skip, edge1, edge2, of, sems,
):
    och = side.shape[0]
    half = wa.shape[0]
    step = 288
    fetch = [
        pltpu.make_async_copy(acc_hbm, acc, sems.at[0]),
        pltpu.make_async_copy(skip_hbm, skip, sems.at[1]),
    ]
    for copy in fetch:
        copy.start()

    def spread(k, _):
        at = pl.multiple_of(k * step, 16)
        for base, part in ((0, wa), (half, wb)):
            got = mm_t(part[pl.ds(at, step), :], lonb[...])
            to = rows_at(base + at, step, 16)
            bands[to, :] = got[:, :128]
            sideb[to, :] = got[:, 128:]
        return 0

    lax.fori_loop(0, half // step, spread, 0)

    def rows(k, _):
        pair = [bands[pl.ds(2 * k + m, 64, stride=WP), :].astype(BF16) for m in range(2)]
        got = mm(latb[pl.ds(0, YP), :], jnp.concatenate(pair, axis=1))
        cf[rows_at(2 * k * YP, YP, 8), :] = got[:, :128]
        cf[rows_at((2 * k + 1) * YP, YP, 8), :] = got[:, 128:]
        return 0

    lax.fori_loop(0, WP // 2, rows, 0, unroll=6)

    lane = iota((64, 128), 1)
    for b in range(CP // 16):
        packed = jnp.zeros((64, 128), F32)
        for c in range(min(16, WP - 16 * b)):
            one = sideb[pl.ds(16 * b + c, 64, stride=WP), :]
            packed = jnp.where(lane // 8 == c, one, packed)
        ch[pl.ds(128 * b, 128), :] = mm_t(packed.T.astype(BF16), latb[...])
    for x in range(6):
        s, k = x // 3, x % 3
        for b in range(CP // 16):
            pc[pl.ds(CP * k + 16 * b, 16), pl.ds(128 * s, 128)] = ch[
                pl.ds(128 * b + x, 16, stride=8), :
            ].astype(BF16)

    def turn(y, _):
        one = cf[pl.ds(y, WP, stride=YP), :]
        one = jnp.concatenate([one, jnp.zeros((CP - WP, 128), F32)], axis=0)
        cs[rows_at(CP * y, CP, 16), :] = one.astype(BF16)
        return 0

    lax.fori_loop(0, 68, turn, 0, unroll=4)

    lane = iota((och, 128), 1)
    got = mm(v1c[...], pc[...])
    for s in range(2):
        lanes = pl.ds(128 * s, 128)
        v = along(got[:, 128 * s : 128 * s + 128], och) + side[:, lanes]
        v = v / (1.0 + jnp.exp(-v))
        keep = (
            ((lane > 0) | (scal[0] > 0))
            & ((lane < 65) | (scal[1] > 0))
            & (lane < 66)
            & (scal[2 + s] > 0)
        )
        v = jnp.where(keep, v, 0.0).astype(BF16)
        edge2[s] = along(mm(stacked(k2, 2 * s, och), v), och)
        edge1[s] = along(mm(e1c[s], pc[pl.ds(CP, CP), lanes]), och)
    for copy in fetch:
        copy.wait()

    def conv1(i, _):
        r = 2 * i
        cond = [cs[rows_at(CP * (r + m), 3 * CP, 16), :] for m in range(2)]
        got = mm(w1c[...], jnp.concatenate(cond, axis=1))
        for m in range(2):
            parts = got[:, 128 * m : 128 * m + 128]
            at = rows_at(och * (r + m), och, 16)
            v = across(parts, edge1, r + m, och) + acc[at, :]
            v = v / (1.0 + jnp.exp(-v))
            live = jnp.where(r + m == 0, scal[0], jnp.where(r + m == 65, scal[1], 1))
            hid[at, :] = (v * live.astype(F32)).astype(BF16)
            skip[at, :] = skip[at, :] + parts[3 * och :]
        return 0

    lax.fori_loop(0, 33, conv1, 0)

    def conv2(j, _):
        y = 2 * j
        above = [hid[rows_at(och * (y + m), 3 * och, 16), :] for m in range(2)]
        got = mm(w2[...], jnp.concatenate(above, axis=1))
        for m in range(2):
            v = across(got[:, 128 * m : 128 * m + 128], edge2, y + m, och)
            of[pl.ds(y + m, och, stride=YP), :] = v + skip[rows_at(och * (y + m + 1), och, 16), :]
        return 0

    lax.fori_loop(0, 32, conv2, 0)

    def leave(o, _):
        out[o] = of[rows_at(YP * o, 64, 8), :].astype(BF16)
        return 0

    lax.fori_loop(0, och, leave, 0, unroll=4)


def pick_body(scal, rows, out):
    lon = rows.shape[2]
    for d in range(8):
        hit = chosen(iota((lon, 128), 0) == iota((lon, 128), 1) + scal[8 + d])
        got = mm(rows[scal[d]], hit)
        out[d] = jnp.concatenate([got, jnp.zeros((WP - got.shape[0], 128), F32)], axis=0).astype(BF16)


def call(body, outs, scratch, args, specs=None, scalars=0, flops=10**7, vmem=48):
    def whole(shape):
        zeros = (0,) * len(shape)
        return pl.BlockSpec(shape, lambda i, *_: zeros, pipeline_mode=pl.Buffered(1))

    specs = specs or {}
    arrays = args[scalars:]
    return pl.pallas_call(
        body,
        grid_spec=pltpu.PrefetchScalarGridSpec(
            num_scalar_prefetch=scalars,
            grid=(1,),
            in_specs=[specs.get(n) or whole(a.shape) for n, a in enumerate(arrays)],
            out_specs=[whole(o.shape) for o in outs],
            scratch_shapes=scratch,
        ),
        out_shape=outs,
        compiler_params=pltpu.CompilerParams(vmem_limit_bytes=vmem * 2**20),
        cost_estimate=pl.CostEstimate(flops=flops, bytes_accessed=2**20, transcendentals=0),
    )(*args)


def out(shape, dtype=BF16):
    return jax.ShapeDtypeStruct(shape, dtype)


def turned_state(state):
    return call(
        turn_body, [out((64 * SP, 128)), out((4 * SP, 128))],
        [pltpu.VMEM((YP * SP, 128), F32), pltpu.VMEM((512, 128), F32)],
        [state], flops=10**9,
    )


def with_corners(scal, strips, above, below):
    return call(
        corner_body, [out((4 * SP, 128))], [], [scal, strips, above, below],
        scalars=1,
    )[0]


def early(scal, xs, above, below, ext, west, east, k1, sw, k2, lon, lat, rho, b1, b2):
    och, cin = sw.shape
    return call(
        early_body,
        [
            out((66 * och, 128), F32), out((66 * och, 128), F32), out((och, 256), F32),
            out((4 * och, 3 * CP)), out((3 * och, 3 * CP)), out((2, 3 * och, CP)),
            out((3 * och, 3 * och)), out((256, 128)), out((128, 64)),
        ],
        [pltpu.VMEM((68 * SP, 128), BF16), pltpu.VMEM((4 * och, 3 * SP), BF16), pltpu.SemaphoreType.DMA],
        [
            scal, xs, above, below, ext, west, east, k1.reshape(3, 3 * och, cin), sw,
            k2.reshape(3, 3 * och, och), lon, lat, rho, b1[None], b2[None],
        ],
        specs={
            0: pl.BlockSpec(memory_space=pltpu.HBM),
            9: pl.BlockSpec((1, 512, 128), lambda i, s: (s[9], 0, 0)),
            10: pl.BlockSpec((1, 512, 64), lambda i, s: (s[10], 0, 0)),
        },
        scalars=1, flops=6 * 10**9,
    )


def late(scal, wa, wb, k2, parts):
    acc, skip, side, w1c, v1c, e1c, w2, lonb, latb = parts
    och = side.shape[0]
    vm = pltpu.VMEM
    return call(
        late_body, [out((och, 64, 128))],
        [
            vm((64 * WP, 128), F32), vm((64 * WP, 128), F32), vm((WP * YP, 128), F32),
            vm((128 * CP // 16, 128), F32), vm((68 * CP, 128), BF16), vm((3 * CP, 256), BF16),
            vm((66 * och, 128), BF16), vm((66 * och, 128), F32), vm((66 * och, 128), F32),
            vm((2, och, 128), F32), vm((2, och, 128), F32), vm((och * YP, 128), F32),
            pltpu.SemaphoreType.DMA((2,)),
        ],
        [
            scal, wa, wb, lonb, latb, w1c, v1c, e1c, w2, k2.reshape(3, 3 * och, och), side, acc, skip,
        ],
        specs={10: pl.BlockSpec(memory_space=pltpu.HBM), 11: pl.BlockSpec(memory_space=pltpu.HBM)},
        scalars=1, flops=8 * 10**9, vmem=58,
    )[0]


def picked(scal, rows):
    return call(pick_body, [out((8, WP, 128))], [], [scal, rows], scalars=1)[0]


def domain_half(tile, tiles, rotation):
    return ((tile + rotation) % tiles) // (tiles // 2)


def routes(regions, tiles, rotation):
    bands = tiles // ROWS
    half = [[domain_half(ROWS * k + g, tiles, rotation) for k in range(bands)] for g in range(ROWS)]
    by_row, by_domain, rows = [], [], np.zeros((tiles, 2), np.int32)
    for z in range(regions):
        for g in range(ROWS):
            by_row.append([z * tiles + k * ROWS + g for k in range(bands)])
    for g in range(ROWS):
        lower = [k for k in range(bands) if half[g][k] == 0]
        upper = [k for k in range(bands) if half[g][k] == 1]
        for pair in zip(lower, upper):
            by_domain.append([z * tiles + k * ROWS + g for z in range(regions) for k in pair])
            for k in pair:
                rows[k * ROWS + g] = [ROWS * g + pair[0], ROWS * g + pair[1]]
    tile_half = [domain_half(t, tiles, rotation) for t in range(tiles)]
    spread, table = [], np.zeros((2, 2, tiles), np.int32)
    for z in range(regions):
        for h in range(2):
            for core in range(2):
                spread.append([z * tiles + t for t in range(tiles) if tile_half[t] == h and t % 2 == core])
    for h in range(2):
        for core in range(2):
            mine = [t for t in range(tiles) if tile_half[t] == h and t % 2 == core]
            other = [t for t in range(tiles) if tile_half[t] == h and t % 2 != core]
            table[h, core] = np.concatenate([rows[t] for t in mine + other])
    return by_row, by_domain, spread, table


def swap(value, groups):
    return lax.all_to_all(
        value, EVERY, split_axis=0, concat_axis=0, axis_index_groups=groups, tiled=True
    )


def from_neighbour(block, distance):
    size = lax.axis_size("tile")
    return lax.ppermute(block, "tile", [((i - distance) % size, i) for i in range(size)])


def shards(
    global_field,
    regional_state,
    windows,
    longitude_weights,
    latitude_weights,
    first_kernel,
    first_bias,
    second_kernel,
    later_conv_bias,
    shortcut_weight,
):
    tile_count, regions = lax.axis_size("tile"), lax.axis_size("region")
    tile, region = lax.axis_index("tile"), lax.axis_index("region")
    half_count = tile_count // 2
    row_tiles = half_count // TCOLS
    rotation = tile_count // 4 + 2
    position = (tile + rotation) % tile_count
    half, within = position // half_count, position % half_count
    row, col = within // TCOLS, within % TCOLS
    domain = 2 * region + half
    by_row, by_domain, spread, table = routes(regions, tile_count, rotation)

    by_rows = swap(global_field.transpose(1, 0, 2), by_row)

    own = lax.dynamic_index_in_dim(windows, domain, 0, keepdims=False)
    flags = [row > 0, row < row_tiles - 1, col > 0, col < TCOLS - 1]
    scal = jnp.stack([*flags, row, col, own[0], own[1], own[3], domain, half]).astype(jnp.int32)
    rho = lax.dynamic_slice(jnp.asarray(table), (half, tile % 2, 0), (1, 1, 64))[0]

    xs, strips = turned_state(regional_state[0])
    above = from_neighbour(xs[-2 * SP :], TCOLS)
    below = from_neighbour(xs[: 2 * SP], -TCOLS)
    ext = with_corners(scal, strips, above, below)
    residue = ROWS * (tile % ROWS) + tile // ROWS
    source = (windows[:, 0] + (residue - windows[:, 0]) % 64) // 64
    offset = windows[:, 2] - global_field.shape[2] * region
    where, ext = lax.optimization_barrier((jnp.concatenate([source, offset]), ext))
    chosen_parts = picked(where, by_rows)
    west = from_neighbour(ext[: 2 * SP], 1)
    east = from_neighbour(ext[2 * SP :], -1)
    parts = early(
        scal, xs, above, below, ext, west, east, first_kernel, shortcut_weight, second_kernel,
        longitude_weights, latitude_weights, rho, first_bias, later_conv_bias,
    )
    mixed = swap(chosen_parts, by_domain)
    piece = mixed.reshape(regions, 2, *mixed.shape[1:]).astype(jnp.float32).sum(0)
    piece = piece.astype(jnp.bfloat16)
    piece, parts = lax.optimization_barrier((piece, parts))
    sharers = len(spread[0])
    mine = swap(jnp.broadcast_to(piece[None], (sharers, *piece.shape)), spread)
    mine = mine.reshape(-1, piece.shape[-1])
    other = lax.ppermute(mine, EVERY, [(i, i ^ 1) for i in range(regions * tile_count)])
    return late(scal, mine, other, second_kernel, parts)[None]


def solution(mesh):
    placed = (
        P(None, "tile", "region"),
        P(("region", "tile"), None, None, None),
        P(),
        P(),
        P("region", None, None),
        P(),
        P(),
        P(),
        P(),
        P(),
    )
    return jax.shard_map(
        shards,
        mesh=mesh,
        in_specs=placed,
        out_specs=P(("region", "tile"), None, None, None),
        check_vma=False,
    )
```

```python
import jax
import jax.numpy as jnp
import numpy as np
from jax import lax
from jax.experimental import pallas as pl
from jax.experimental.pallas import tpu as pltpu
from jax.sharding import PartitionSpec as P


TCOLS = 4
ROWS = 8
EVERY = ("region", "tile")
SP = 112
CP = 80
WP = 72
YP = 72
F32, BF16 = jnp.float32, jnp.bfloat16


def mm(a, b):
    return jnp.dot(a, b, preferred_element_type=F32)


def mm_t(a, b):
    return lax.dot_general(a, b, (((1,), (1,)), ((), ())), preferred_element_type=F32)


def iota(shape, dim):
    return lax.broadcasted_iota(jnp.int32, shape, dim)


def chosen(cond):
    return jnp.where(cond, 1.0, 0.0).astype(BF16)


def column(row):
    n = row.shape[1]
    hit = iota((n, n), 0) == iota((n, n), 1)
    return jnp.sum(jnp.where(hit, row, 0.0), axis=1, keepdims=True)


def rows_at(start, size, unit):
    return pl.ds(pl.multiple_of(start, unit), size)


def along(parts, och):
    return (
        parts[:och]
        + pltpu.roll(parts[och : 2 * och], 127, 1)
        + pltpu.roll(parts[2 * och : 3 * och], 126, 1)
    )


def across(parts, edges, at, och):
    lane = iota((och, 128), 1)
    west = jnp.where(lane == 0, pltpu.roll(edges[0], 128 - at, 1), pltpu.roll(parts[:och], 1, 1))
    east = jnp.where(
        lane == 127, pltpu.roll(edges[1], 127 - at, 1), pltpu.roll(parts[2 * och : 3 * och], 127, 1)
    )
    return parts[och : 2 * och] + west + east


def stacked(k3, q, och):
    return jnp.concatenate([k3[p, q * och : (q + 1) * och, :] for p in range(3)], axis=0)


def paired(count, mix, end, even, odd):
    mix(0, even)

    def two(i, _):
        mix(8 * i + 4, odd)
        end(8 * i, even)
        mix(8 * i + 8, even)
        end(8 * i + 4, odd)
        return 0

    lax.fori_loop(0, (count - 1) // 2, two, 0)
    if count % 2 == 0:
        mix(4 * count - 4, odd)
        end(4 * count - 8, even)
        end(4 * count - 4, odd)
    else:
        end(4 * count - 4, even)


def turn_body(state, xs, strips, flat, packs):
    chans, height = state.shape[0], state.shape[1]

    def widen(c, _):
        flat[rows_at(YP * c, height, 8), :] = state[c].astype(F32)
        return 0

    lax.fori_loop(0, chans, widen, 0, unroll=3)
    flat[pl.ds(YP * chans, YP * (SP - chans)), :] = jnp.zeros((YP * (SP - chans), 128), F32)

    def row(y, _):
        xs[rows_at(SP * y, SP, 16), :] = flat[pl.ds(y, SP, stride=YP), :].astype(BF16)
        return 0

    lax.fori_loop(0, height, row, 0, unroll=4)
    lane = iota((height, 128), 1)
    for b in range(4):
        packed = jnp.zeros((height, 128), F32)
        for c in range(min(32, chans - 32 * b)):
            one = pltpu.roll(flat[pl.ds(YP * (32 * b + c), height), :], (2 + 4 * c) % 128, 1)
            packed = jnp.where(lane // 4 == c, one, packed)
        packed = jnp.concatenate([packed, jnp.zeros((128 - height, 128), F32)], axis=0)
        packs[pl.ds(128 * b, 128), :] = packed.T
    for col in range(4):
        for b in range(4):
            n = min(32, SP - 32 * b)
            strips[pl.ds(SP * col + 32 * b, n), :] = packs[
                pl.ds(128 * b + col, n, stride=4), :
            ].astype(BF16)


def corner_body(scal, strips, above, below, ext):
    lane = iota((SP, 128), 1)
    top, bottom = scal[0] > 0, scal[1] > 0
    for j, x in enumerate((126, 127, 0, 1)):
        e = pltpu.roll(strips[pl.ds(SP * j, SP), :].astype(F32), 2, 1)
        for m in range(2):
            up = pltpu.roll(above[pl.ds(SP * m, SP), :].astype(F32), (m - x) % 128, 1)
            down = pltpu.roll(below[pl.ds(SP * m, SP), :].astype(F32), (66 + m - x) % 128, 1)
            e = jnp.where((lane == m) & top, up, e)
            e = jnp.where((lane == 66 + m) & bottom, down, e)
        ext[pl.ds(SP * j, SP), :] = e.astype(BF16)


def early_body(
    scal, xs_own, above, below, ext, west, east, k1, sw, k2, lon, lat, rho, b1, b2,
    acc, skip, side, w1c, v1c, e1c, w2, lonb, latb,
    xs, w1s, wide1, wide2, even, odd, sem,
):
    och = sw.shape[0]
    cin = sw.shape[1]
    sch = cin - 70
    fetch = pltpu.make_async_copy(xs_own, xs.at[pl.ds(2 * SP, 64 * SP)], sem)
    fetch.start()
    top, bottom, left, right = scal[0] > 0, scal[1] > 0, scal[2] > 0, scal[3] > 0
    xs[pl.ds(0, 2 * SP), :] = jnp.where(top, above[...], 0)
    xs[pl.ds(66 * SP, 2 * SP), :] = jnp.where(bottom, below[...], 0)
    bias1, bias2 = column(b1[...]), column(b2[...])
    wide1[...] = jnp.broadcast_to(bias1, wide1.shape)
    wide2[...] = jnp.broadcast_to(bias2, wide2.shape)
    xs[pl.ds(68 * SP, 2 * SP), :] = jnp.zeros((2 * SP, 128), BF16)

    row_s, col_s = iota((cin, 3 * SP), 0), iota((cin, 3 * SP), 1)
    row_c, col_c = iota((cin, 3 * CP), 0), iota((cin, 3 * CP), 1)
    put_s = [chosen((col_s == SP * p + row_s) & (row_s < sch)) for p in range(3)]
    put_c = [chosen((col_c == CP * p + row_c - sch) & (row_c >= sch)) for p in range(3)]
    w1s[pl.ds(0, 3 * och), :] = sum(mm(k1[p], put_s[p]) for p in range(3)).astype(BF16)
    w1s[pl.ds(3 * och, och), :] = mm(sw[...], put_s[1]).astype(BF16)
    w1c[pl.ds(0, 3 * och), :] = sum(mm(k1[p], put_c[p]) for p in range(3)).astype(BF16)
    w1c[pl.ds(3 * och, och), :] = mm(sw[...], put_c[1]).astype(BF16)
    turned = [stacked(k1, q, och) for q in range(3)]
    v1s = sum(mm(turned[q], put_s[q]) for q in range(3)).astype(BF16)
    v1c[...] = sum(mm(turned[q], put_c[q]) for q in range(3)).astype(BF16)
    row_e, col_e = iota((cin, CP), 0), iota((cin, CP), 1)
    put_e = chosen((col_e == row_e - sch) & (row_e >= sch))
    e1c[0] = mm(turned[0], put_e).astype(BF16)
    e1c[1] = mm(turned[2], put_e).astype(BF16)
    row_2, col_2 = iota((och, 3 * och), 0), iota((och, 3 * och), 1)
    w2[...] = sum(mm(k2[p], chosen(col_2 == och * p + row_2)) for p in range(3)).astype(BF16)

    masked = jnp.where(iota((512, 128), 1) < scal[8], lon[0], 0)
    r, c = iota((256, 512), 0), iota((256, 512), 1)
    six = (r - 128) % 8
    off = jnp.where(r < 128, r, jnp.where(six < 3, six - 2, six + 124))
    pick = chosen((c == off + 128 * scal[5]) & ((r < 128) | (six < 6)))
    lonb[...] = mm(pick, masked).astype(BF16)
    r, c = iota((128, 512), 0), iota((128, 512), 1)
    pick = chosen((c == r - 2 + 64 * scal[4]) & (r < 68))
    taken = mm(pick, lat[0]).astype(BF16)
    want = (rho[...] - scal[6]) & 63
    order = chosen((iota((64, 64), 0) == want) & (want < scal[7]))
    latb[...] = mm(taken, order).astype(BF16)

    west_in = jnp.where(left, west[...], 0)
    east_in = jnp.where(right, east[...], 0)
    ps = jnp.concatenate(
        [
            jnp.concatenate([west_in, ext[pl.ds(2 * SP, SP), :]], axis=0),
            jnp.concatenate([ext[pl.ds(SP, SP), :], east_in], axis=0),
        ],
        axis=1,
    )
    got = mm(v1s, ps)
    for s in range(2):
        side[:, 128 * s : 128 * s + 128] = along(got[:, 128 * s : 128 * s + 128], och) + bias1
    edges = [
        along(mm(turned[0][:, :SP], west_in[SP:]), och),
        along(mm(turned[2][:, :SP], east_in[:SP]), och),
    ]
    fetch.wait()

    def mix(r, to):
        rows = [xs[rows_at(SP * (r + m), 3 * SP, 16), :] for m in range(4)]
        to[...] = mm(w1s[...], jnp.concatenate(rows, axis=1))

    def end(r, got):
        for m in range(4):
            parts = got[:, 128 * m : 128 * m + 128]
            at = rows_at(och * (r + m), och, 16)
            acc[at, :] = across(parts, edges, r + m, och) + wide1[...]
            skip[at, :] = parts[3 * och :] + wide2[...]

    paired(17, mix, end, even, odd)


def late_body(
    scal, wa, wb, lonb, latb, w1c, v1c, e1c, w2, k2, side, acc_hbm, skip_hbm,
    out, bands, sideb, cf, ch, cs, pc, hid, acc, skip, edge1, edge2, of, even, odd, sems,
):
    och = side.shape[0]
    half = wa.shape[0]
    step = 288
    fetch = [
        pltpu.make_async_copy(acc_hbm, acc, sems.at[0]),
        pltpu.make_async_copy(skip_hbm, skip, sems.at[1]),
    ]
    for copy in fetch:
        copy.start()

    def spread(k, _):
        at = pl.multiple_of(k * step, 16)
        for base, part in ((0, wa), (half, wb)):
            got = mm_t(part[pl.ds(at, step), :], lonb[...])
            to = rows_at(base + at, step, 16)
            bands[to, :] = got[:, :128]
            sideb[to, :] = got[:, 128:]
        return 0

    lax.fori_loop(0, half // step, spread, 0)

    def rows(k, _):
        pair = [bands[pl.ds(2 * k + m, 64, stride=WP), :].astype(BF16) for m in range(2)]
        got = mm(latb[pl.ds(0, YP), :], jnp.concatenate(pair, axis=1))
        cf[rows_at(2 * k * YP, YP, 8), :] = got[:, :128]
        cf[rows_at((2 * k + 1) * YP, YP, 8), :] = got[:, 128:]
        return 0

    lax.fori_loop(0, WP // 2, rows, 0, unroll=6)

    lane = iota((64, 128), 1)
    for b in range(CP // 16):
        packed = jnp.zeros((64, 128), F32)
        for c in range(min(16, WP - 16 * b)):
            one = sideb[pl.ds(16 * b + c, 64, stride=WP), :]
            packed = jnp.where(lane // 8 == c, one, packed)
        ch[pl.ds(128 * b, 128), :] = mm_t(packed.T.astype(BF16), latb[...])
    for x in range(6):
        s, k = x // 3, x % 3
        for b in range(CP // 16):
            pc[pl.ds(CP * k + 16 * b, 16), pl.ds(128 * s, 128)] = ch[
                pl.ds(128 * b + x, 16, stride=8), :
            ].astype(BF16)

    def turn(y, _):
        one = cf[pl.ds(y, WP, stride=YP), :]
        one = jnp.concatenate([one, jnp.zeros((CP - WP, 128), F32)], axis=0)
        cs[rows_at(CP * y, CP, 16), :] = one.astype(BF16)
        return 0

    lax.fori_loop(0, 68, turn, 0, unroll=4)
    cs[pl.ds(68 * CP, 2 * CP), :] = jnp.zeros((2 * CP, 128), BF16)

    lane = iota((och, 128), 1)
    got = mm(v1c[...], pc[...])
    for s in range(2):
        lanes = pl.ds(128 * s, 128)
        v = along(got[:, 128 * s : 128 * s + 128], och) + side[:, lanes]
        v = v / (1.0 + jnp.exp(-v))
        keep = (
            ((lane > 0) | (scal[0] > 0))
            & ((lane < 65) | (scal[1] > 0))
            & (lane < 66)
            & (scal[2 + s] > 0)
        )
        v = jnp.where(keep, v, 0.0).astype(BF16)
        edge2[s] = along(mm(stacked(k2, 2 * s, och), v), och)
        edge1[s] = along(mm(e1c[s], pc[pl.ds(CP, CP), lanes]), och)
    for copy in fetch:
        copy.wait()

    def window(ref, unit, r):
        return jnp.concatenate(
            [ref[rows_at(unit * (r + m), 3 * unit, 16), :] for m in range(4)], axis=1
        )

    def mix1(r, to):
        to[...] = mm(w1c[...], window(cs, CP, r))

    def end1(r, got):
        for m in range(4):
            parts = got[:, 128 * m : 128 * m + 128]
            at = rows_at(och * (r + m), och, 16)
            v = across(parts, edge1, r + m, och) + acc[at, :]
            v = v / (1.0 + jnp.exp(-v))
            live = jnp.where(r + m == 0, scal[0], jnp.where(r + m == 65, scal[1], 1))
            hid[at, :] = (v * live.astype(F32)).astype(BF16)
            skip[at, :] = skip[at, :] + parts[3 * och :]

    def mix2(y, to):
        to[pl.ds(0, 3 * och), :] = mm(w2[...], window(hid, och, y))

    def end2(y, got):
        for m in range(4):
            v = across(got[:, 128 * m : 128 * m + 128], edge2, y + m, och)
            of[pl.ds(y + m, och, stride=YP), :] = v + skip[rows_at(och * (y + m + 1), och, 16), :]

    paired(17, mix1, end1, even, odd)
    paired(16, mix2, end2, even, odd)

    def leave(o, _):
        out[o] = of[rows_at(YP * o, 64, 8), :].astype(BF16)
        return 0

    lax.fori_loop(0, och, leave, 0, unroll=4)


def pick_body(scal, rows, out):
    lon = rows.shape[2]
    for d in range(8):
        hit = chosen(iota((lon, 128), 0) == iota((lon, 128), 1) + scal[8 + d])
        got = mm(rows[scal[d]], hit)
        out[d] = jnp.concatenate([got, jnp.zeros((WP - got.shape[0], 128), F32)], axis=0).astype(BF16)


def call(body, outs, scratch, args, specs=None, scalars=0, flops=10**7, vmem=48):
    def whole(shape):
        zeros = (0,) * len(shape)
        return pl.BlockSpec(shape, lambda i, *_: zeros, pipeline_mode=pl.Buffered(1))

    specs = specs or {}
    arrays = args[scalars:]
    return pl.pallas_call(
        body,
        grid_spec=pltpu.PrefetchScalarGridSpec(
            num_scalar_prefetch=scalars,
            grid=(1,),
            in_specs=[specs.get(n) or whole(a.shape) for n, a in enumerate(arrays)],
            out_specs=[whole(o.shape) for o in outs],
            scratch_shapes=scratch,
        ),
        out_shape=outs,
        compiler_params=pltpu.CompilerParams(vmem_limit_bytes=vmem * 2**20),
        cost_estimate=pl.CostEstimate(flops=flops, bytes_accessed=2**20, transcendentals=0),
    )(*args)


def out(shape, dtype=BF16):
    return jax.ShapeDtypeStruct(shape, dtype)


def turned_state(state):
    return call(
        turn_body, [out((64 * SP, 128)), out((4 * SP, 128))],
        [pltpu.VMEM((YP * SP, 128), F32), pltpu.VMEM((512, 128), F32)],
        [state], flops=10**9,
    )


def with_corners(scal, strips, above, below):
    return call(
        corner_body, [out((4 * SP, 128))], [], [scal, strips, above, below],
        scalars=1,
    )[0]


def early(scal, xs, above, below, ext, west, east, k1, sw, k2, lon, lat, rho, b1, b2):
    och, cin = sw.shape
    return call(
        early_body,
        [
            out((68 * och, 128), F32), out((68 * och, 128), F32), out((och, 256), F32),
            out((4 * och, 3 * CP)), out((3 * och, 3 * CP)), out((2, 3 * och, CP)),
            out((3 * och, 3 * och)), out((256, 128)), out((128, 64)),
        ],
        [
            pltpu.VMEM((70 * SP, 128), BF16), pltpu.VMEM((4 * och, 3 * SP), BF16),
            pltpu.VMEM((och, 128), F32), pltpu.VMEM((och, 128), F32),
            pltpu.VMEM((4 * och, 512), F32), pltpu.VMEM((4 * och, 512), F32),
            pltpu.SemaphoreType.DMA,
        ],
        [
            scal, xs, above, below, ext, west, east, k1.reshape(3, 3 * och, cin), sw,
            k2.reshape(3, 3 * och, och), lon, lat, rho, b1[None], b2[None],
        ],
        specs={
            0: pl.BlockSpec(memory_space=pltpu.HBM),
            9: pl.BlockSpec((1, 512, 128), lambda i, s: (s[9], 0, 0)),
            10: pl.BlockSpec((1, 512, 64), lambda i, s: (s[10], 0, 0)),
        },
        scalars=1, flops=6 * 10**9,
    )


def late(scal, wa, wb, k2, parts):
    acc, skip, side, w1c, v1c, e1c, w2, lonb, latb = parts
    och = side.shape[0]
    vm = pltpu.VMEM
    return call(
        late_body, [out((och, 64, 128))],
        [
            vm((64 * WP, 128), F32), vm((64 * WP, 128), F32), vm((WP * YP, 128), F32),
            vm((128 * CP // 16, 128), F32), vm((70 * CP, 128), BF16), vm((3 * CP, 256), BF16),
            vm((68 * och, 128), BF16), vm((68 * och, 128), F32), vm((68 * och, 128), F32),
            vm((2, och, 128), F32), vm((2, och, 128), F32), vm((och * YP, 128), F32),
            vm((4 * och, 512), F32), vm((4 * och, 512), F32), pltpu.SemaphoreType.DMA((2,)),
        ],
        [
            scal, wa, wb, lonb, latb, w1c, v1c, e1c, w2, k2.reshape(3, 3 * och, och), side, acc, skip,
        ],
        specs={10: pl.BlockSpec(memory_space=pltpu.HBM), 11: pl.BlockSpec(memory_space=pltpu.HBM)},
        scalars=1, flops=8 * 10**9, vmem=40,
    )[0]


def picked(scal, rows):
    return call(pick_body, [out((8, WP, 128))], [], [scal, rows], scalars=1)[0]


def domain_half(tile, tiles, rotation):
    return ((tile + rotation) % tiles) // (tiles // 2)


def routes(regions, tiles, rotation):
    bands = tiles // ROWS
    half = [[domain_half(ROWS * k + g, tiles, rotation) for k in range(bands)] for g in range(ROWS)]
    by_row, by_domain, rows = [], [], np.zeros((tiles, 2), np.int32)
    for z in range(regions):
        for g in range(ROWS):
            by_row.append([z * tiles + k * ROWS + g for k in range(bands)])
    for g in range(ROWS):
        lower = [k for k in range(bands) if half[g][k] == 0]
        upper = [k for k in range(bands) if half[g][k] == 1]
        for pair in zip(lower, upper):
            by_domain.append([z * tiles + k * ROWS + g for z in range(regions) for k in pair])
            for k in pair:
                rows[k * ROWS + g] = [ROWS * g + pair[0], ROWS * g + pair[1]]
    tile_half = [domain_half(t, tiles, rotation) for t in range(tiles)]
    spread, table = [], np.zeros((2, 2, tiles), np.int32)
    for z in range(regions):
        for h in range(2):
            for core in range(2):
                spread.append([z * tiles + t for t in range(tiles) if tile_half[t] == h and t % 2 == core])
    for h in range(2):
        for core in range(2):
            mine = [t for t in range(tiles) if tile_half[t] == h and t % 2 == core]
            other = [t for t in range(tiles) if tile_half[t] == h and t % 2 != core]
            table[h, core] = np.concatenate([rows[t] for t in mine + other])
    return by_row, by_domain, spread, table


def swap(value, groups):
    return lax.all_to_all(
        value, EVERY, split_axis=0, concat_axis=0, axis_index_groups=groups, tiled=True
    )


def from_neighbour(block, distance):
    size = lax.axis_size("tile")
    return lax.ppermute(block, "tile", [((i - distance) % size, i) for i in range(size)])


def shards(
    global_field,
    regional_state,
    windows,
    longitude_weights,
    latitude_weights,
    first_kernel,
    first_bias,
    second_kernel,
    later_conv_bias,
    shortcut_weight,
):
    tile_count, regions = lax.axis_size("tile"), lax.axis_size("region")
    tile, region = lax.axis_index("tile"), lax.axis_index("region")
    half_count = tile_count // 2
    row_tiles = half_count // TCOLS
    rotation = tile_count // 4 + 2
    position = (tile + rotation) % tile_count
    half, within = position // half_count, position % half_count
    row, col = within // TCOLS, within % TCOLS
    domain = 2 * region + half
    by_row, by_domain, spread, table = routes(regions, tile_count, rotation)

    by_rows = swap(global_field.transpose(1, 0, 2), by_row)

    own = lax.dynamic_index_in_dim(windows, domain, 0, keepdims=False)
    flags = [row > 0, row < row_tiles - 1, col > 0, col < TCOLS - 1]
    scal = jnp.stack([*flags, row, col, own[0], own[1], own[3], domain, half]).astype(jnp.int32)
    rho = lax.dynamic_slice(jnp.asarray(table), (half, tile % 2, 0), (1, 1, 64))[0]

    xs, strips = turned_state(regional_state[0])
    above = from_neighbour(xs[-2 * SP :], TCOLS)
    below = from_neighbour(xs[: 2 * SP], -TCOLS)
    residue = ROWS * (tile % ROWS) + tile // ROWS
    source = (windows[:, 0] + (residue - windows[:, 0]) % 64) // 64
    offset = windows[:, 2] - global_field.shape[2] * region
    where, above, below = lax.optimization_barrier(
        (jnp.concatenate([source, offset]), above, below)
    )
    chosen_parts = picked(where, by_rows)
    ext = with_corners(scal, strips, above, below)
    west = from_neighbour(ext[: 2 * SP], 1)
    east = from_neighbour(ext[2 * SP :], -1)
    mixed = swap(chosen_parts, by_domain)
    piece = mixed.reshape(regions, 2, *mixed.shape[1:]).astype(jnp.float32).sum(0)
    piece = piece.astype(jnp.bfloat16)
    piece, west, east = lax.optimization_barrier((piece, west, east))
    parts = early(
        scal, xs, above, below, ext, west, east, first_kernel, shortcut_weight, second_kernel,
        longitude_weights, latitude_weights, rho, first_bias, later_conv_bias,
    )
    sharers = len(spread[0])
    mine = swap(jnp.broadcast_to(piece[None], (sharers, *piece.shape)), spread)
    mine = mine.reshape(-1, piece.shape[-1])
    other = lax.ppermute(mine, EVERY, [(i, i ^ 1) for i in range(regions * tile_count)])
    return late(scal, mine, other, second_kernel, parts)[None]


def solution(mesh):
    placed = (
        P(None, "tile", "region"),
        P(("region", "tile"), None, None, None),
        P(),
        P(),
        P("region", None, None),
        P(),
        P(),
        P(),
        P(),
        P(),
    )
    return jax.shard_map(
        shards,
        mesh=mesh,
        in_specs=placed,
        out_specs=P(("region", "tile"), None, None, None),
        check_vma=False,
    )
```

```python
import jax
import jax.numpy as jnp
import numpy as np
from jax import lax
from jax.experimental import pallas as pl
from jax.experimental.pallas import tpu as pltpu
from jax.sharding import PartitionSpec as P


TCOLS = 4
ROWS = 8
EVERY = ("region", "tile")
SP = 112
CP = 80
WP = 72
YP = 72
F32, BF16 = jnp.float32, jnp.bfloat16


def mm(a, b):
    return jnp.dot(a, b, preferred_element_type=F32)


def mm_t(a, b):
    return lax.dot_general(a, b, (((1,), (1,)), ((), ())), preferred_element_type=F32)


def iota(shape, dim):
    return lax.broadcasted_iota(jnp.int32, shape, dim)


def chosen(cond):
    return jnp.where(cond, 1.0, 0.0).astype(BF16)


def column(row):
    n = row.shape[1]
    hit = iota((n, n), 0) == iota((n, n), 1)
    return jnp.sum(jnp.where(hit, row, 0.0), axis=1, keepdims=True)


def rows_at(start, size, unit):
    return pl.ds(pl.multiple_of(start, unit), size)


def along(parts, och):
    return (
        parts[:och]
        + pltpu.roll(parts[och : 2 * och], 127, 1)
        + pltpu.roll(parts[2 * och : 3 * och], 126, 1)
    )


def across(parts, edges, at, och):
    lane = iota((och, 128), 1)
    west = jnp.where(lane == 0, pltpu.roll(edges[0], 128 - at, 1), pltpu.roll(parts[:och], 1, 1))
    east = jnp.where(
        lane == 127, pltpu.roll(edges[1], 127 - at, 1), pltpu.roll(parts[2 * och : 3 * och], 127, 1)
    )
    return parts[och : 2 * och] + west + east


def stacked(k3, q, och):
    return jnp.concatenate([k3[p, q * och : (q + 1) * och, :] for p in range(3)], axis=0)


def paired(count, mix, end, even, odd):
    mix(0, even)

    def two(i, _):
        mix(8 * i + 4, odd)
        end(8 * i, even)
        mix(8 * i + 8, even)
        end(8 * i + 4, odd)
        return 0

    lax.fori_loop(0, (count - 1) // 2, two, 0)
    if count % 2 == 0:
        mix(4 * count - 4, odd)
        end(4 * count - 8, even)
        end(4 * count - 4, odd)
    else:
        end(4 * count - 4, even)


def turn_body(state, xs, strips, flat, packs):
    chans, height = state.shape[0], state.shape[1]

    def widen(c, _):
        flat[rows_at(YP * c, height, 8), :] = state[c].astype(F32)
        return 0

    lax.fori_loop(0, chans, widen, 0, unroll=3)
    flat[pl.ds(YP * chans, YP * (SP - chans)), :] = jnp.zeros((YP * (SP - chans), 128), F32)

    def row(y, _):
        xs[rows_at(SP * y, SP, 16), :] = flat[pl.ds(y, SP, stride=YP), :].astype(BF16)
        return 0

    lax.fori_loop(0, height, row, 0, unroll=4)
    lane = iota((height, 128), 1)
    for b in range(4):
        packed = jnp.zeros((height, 128), F32)
        for c in range(min(32, chans - 32 * b)):
            one = pltpu.roll(flat[pl.ds(YP * (32 * b + c), height), :], (2 + 4 * c) % 128, 1)
            packed = jnp.where(lane // 4 == c, one, packed)
        packed = jnp.concatenate([packed, jnp.zeros((128 - height, 128), F32)], axis=0)
        packs[pl.ds(128 * b, 128), :] = packed.T
    for col in range(4):
        for b in range(4):
            n = min(32, SP - 32 * b)
            strips[pl.ds(SP * col + 32 * b, n), :] = packs[
                pl.ds(128 * b + col, n, stride=4), :
            ].astype(BF16)


def corner_body(scal, strips, above, below, ext):
    lane = iota((SP, 128), 1)
    top, bottom = scal[0] > 0, scal[1] > 0
    for j, x in enumerate((126, 127, 0, 1)):
        e = pltpu.roll(strips[pl.ds(SP * j, SP), :].astype(F32), 2, 1)
        for m in range(2):
            up = pltpu.roll(above[pl.ds(SP * m, SP), :].astype(F32), (m - x) % 128, 1)
            down = pltpu.roll(below[pl.ds(SP * m, SP), :].astype(F32), (66 + m - x) % 128, 1)
            e = jnp.where((lane == m) & top, up, e)
            e = jnp.where((lane == 66 + m) & bottom, down, e)
        ext[pl.ds(SP * j, SP), :] = e.astype(BF16)


def pack_body(
    scal, k1, sw, k2, lon, lat, rho, b1, b2,
    w1s, v1s, w1c, v1c, e1c, w2, lonb, latb, wide1, wide2,
):
    och, cin = sw.shape
    sch = cin - 70
    wide1[...] = jnp.broadcast_to(column(b1[...]), wide1.shape)
    wide2[...] = jnp.broadcast_to(column(b2[...]), wide2.shape)
    row_s, col_s = iota((cin, 3 * SP), 0), iota((cin, 3 * SP), 1)
    row_c, col_c = iota((cin, 3 * CP), 0), iota((cin, 3 * CP), 1)
    put_s = [chosen((col_s == SP * p + row_s) & (row_s < sch)) for p in range(3)]
    put_c = [chosen((col_c == CP * p + row_c - sch) & (row_c >= sch)) for p in range(3)]
    w1s[pl.ds(0, 3 * och), :] = sum(mm(k1[p], put_s[p]) for p in range(3)).astype(BF16)
    w1s[pl.ds(3 * och, och), :] = mm(sw[...], put_s[1]).astype(BF16)
    w1c[pl.ds(0, 3 * och), :] = sum(mm(k1[p], put_c[p]) for p in range(3)).astype(BF16)
    w1c[pl.ds(3 * och, och), :] = mm(sw[...], put_c[1]).astype(BF16)
    turned = [stacked(k1, q, och) for q in range(3)]
    v1s[...] = sum(mm(turned[q], put_s[q]) for q in range(3)).astype(BF16)
    v1c[...] = sum(mm(turned[q], put_c[q]) for q in range(3)).astype(BF16)
    row_e, col_e = iota((cin, CP), 0), iota((cin, CP), 1)
    put_e = chosen((col_e == row_e - sch) & (row_e >= sch))
    e1c[0] = mm(turned[0], put_e).astype(BF16)
    e1c[1] = mm(turned[2], put_e).astype(BF16)
    row_2, col_2 = iota((och, 3 * och), 0), iota((och, 3 * och), 1)
    w2[...] = sum(mm(k2[p], chosen(col_2 == och * p + row_2)) for p in range(3)).astype(BF16)

    masked = jnp.where(iota((512, 128), 1) < scal[8], lon[0], 0)
    r, c = iota((256, 512), 0), iota((256, 512), 1)
    six = (r - 128) % 8
    off = jnp.where(r < 128, r, jnp.where(six < 3, six - 2, six + 124))
    pick = chosen((c == off + 128 * scal[5]) & ((r < 128) | (six < 6)))
    lonb[...] = mm(pick, masked).astype(BF16)
    r, c = iota((128, 512), 0), iota((128, 512), 1)
    pick = chosen((c == r - 2 + 64 * scal[4]) & (r < 68))
    taken = mm(pick, lat[0]).astype(BF16)
    want = (rho[...] - scal[6]) & 63
    order = chosen((iota((64, 64), 0) == want) & (want < scal[7]))
    latb[...] = mm(taken, order).astype(BF16)


def early_body(
    scal, xs_own, above, below, ext, west, east, k1, w1s, v1s, wide1, wide2,
    acc, skip, side,
    xs, even, odd, sem,
):
    och = side.shape[0]
    fetch = pltpu.make_async_copy(xs_own, xs.at[pl.ds(2 * SP, 64 * SP)], sem)
    fetch.start()
    top, bottom, left, right = scal[0] > 0, scal[1] > 0, scal[2] > 0, scal[3] > 0
    xs[pl.ds(0, 2 * SP), :] = jnp.where(top, above[...], 0)
    xs[pl.ds(66 * SP, 2 * SP), :] = jnp.where(bottom, below[...], 0)
    xs[pl.ds(68 * SP, 2 * SP), :] = jnp.zeros((2 * SP, 128), BF16)

    west_in = jnp.where(left, west[...], 0)
    east_in = jnp.where(right, east[...], 0)
    ps = jnp.concatenate(
        [
            jnp.concatenate([west_in, ext[pl.ds(2 * SP, SP), :]], axis=0),
            jnp.concatenate([ext[pl.ds(SP, SP), :], east_in], axis=0),
        ],
        axis=1,
    )
    got = mm(v1s[...], ps)
    for s in range(2):
        side[:, 128 * s : 128 * s + 128] = along(got[:, 128 * s : 128 * s + 128], och) + wide1[...]
    edges = [
        along(mm(stacked(k1, 0, och)[:, :SP], west_in[SP:]), och),
        along(mm(stacked(k1, 2, och)[:, :SP], east_in[:SP]), och),
    ]
    fetch.wait()

    def mix(r, to):
        rows = [xs[rows_at(SP * (r + m), 3 * SP, 16), :] for m in range(4)]
        to[...] = mm(w1s[...], jnp.concatenate(rows, axis=1))

    def end(r, got):
        for m in range(4):
            parts = got[:, 128 * m : 128 * m + 128]
            at = rows_at(och * (r + m), och, 16)
            acc[at, :] = across(parts, edges, r + m, och) + wide1[...]
            skip[at, :] = parts[3 * och :] + wide2[...]

    paired(17, mix, end, even, odd)


def total_body(mixed, out):
    piece = mixed[0].astype(F32)
    for z in range(1, mixed.shape[0]):
        piece = piece + mixed[z].astype(F32)
    piece = piece.astype(BF16)
    for n in range(out.shape[0]):
        out[n] = piece


def late_body(
    scal, wa, wb, lonb, latb, w1c, v1c, e1c, w2, k2, side, acc_far, skip_far,
    out, bands, sideb, cf, ch, cs, pc, hid, acc, skip, more, edge1, edge2, of, even, odd, sems,
):
    och = side.shape[0]
    half = wa.shape[0]
    step = 288
    fetch = [
        pltpu.make_async_copy(acc_far, acc, sems.at[0]),
        pltpu.make_async_copy(skip_far, skip, sems.at[1]),
    ]
    for copy in fetch:
        copy.start()

    def spread(k, _):
        at = pl.multiple_of(k * step, 16)
        for base, part in ((0, wa), (half, wb)):
            got = mm_t(part[pl.ds(at, step), :], lonb[...])
            to = rows_at(base + at, step, 16)
            bands[to, :] = got[:, :128]
            sideb[to, :] = got[:, 128:]
        return 0

    lax.fori_loop(0, half // step, spread, 0)

    def rows(k, _):
        pair = [bands[pl.ds(2 * k + m, 64, stride=WP), :].astype(BF16) for m in range(2)]
        got = mm(latb[pl.ds(0, YP), :], jnp.concatenate(pair, axis=1))
        cf[rows_at(2 * k * YP, YP, 8), :] = got[:, :128]
        cf[rows_at((2 * k + 1) * YP, YP, 8), :] = got[:, 128:]
        return 0

    lax.fori_loop(0, WP // 2, rows, 0, unroll=6)

    lane = iota((64, 128), 1)
    for b in range(CP // 16):
        packed = jnp.zeros((64, 128), F32)
        for c in range(min(16, WP - 16 * b)):
            one = sideb[pl.ds(16 * b + c, 64, stride=WP), :]
            packed = jnp.where(lane // 8 == c, one, packed)
        ch[pl.ds(128 * b, 128), :] = mm_t(packed.T.astype(BF16), latb[...])
    for x in range(6):
        s, k = x // 3, x % 3
        for b in range(CP // 16):
            pc[pl.ds(CP * k + 16 * b, 16), pl.ds(128 * s, 128)] = ch[
                pl.ds(128 * b + x, 16, stride=8), :
            ].astype(BF16)

    def turn(y, _):
        one = cf[pl.ds(y, WP, stride=YP), :]
        one = jnp.concatenate([one, jnp.zeros((CP - WP, 128), F32)], axis=0)
        cs[rows_at(CP * y, CP, 16), :] = one.astype(BF16)
        return 0

    lax.fori_loop(0, 68, turn, 0, unroll=4)
    cs[pl.ds(68 * CP, 2 * CP), :] = jnp.zeros((2 * CP, 128), BF16)

    lane = iota((och, 128), 1)
    got = mm(v1c[...], pc[...])
    for s in range(2):
        lanes = pl.ds(128 * s, 128)
        v = along(got[:, 128 * s : 128 * s + 128], och) + side[:, lanes]
        v = v / (1.0 + jnp.exp(-v))
        keep = (
            ((lane > 0) | (scal[0] > 0))
            & ((lane < 65) | (scal[1] > 0))
            & (lane < 66)
            & (scal[2 + s] > 0)
        )
        v = jnp.where(keep, v, 0.0).astype(BF16)
        edge2[s] = along(mm(stacked(k2, 2 * s, och), v), och)
        edge1[s] = along(mm(e1c[s], pc[pl.ds(CP, CP), lanes]), och)
    for copy in fetch:
        copy.wait()

    def window(ref, unit, r):
        return jnp.concatenate(
            [ref[rows_at(unit * (r + m), 3 * unit, 16), :] for m in range(4)], axis=1
        )

    def mix1(r, to):
        to[...] = mm(w1c[...], window(cs, CP, r))

    def end1(r, got):
        for m in range(4):
            parts = got[:, 128 * m : 128 * m + 128]
            at = rows_at(och * (r + m), och, 16)
            v = across(parts, edge1, r + m, och) + acc[at, :]
            v = v / (1.0 + jnp.exp(-v))
            live = jnp.where(r + m == 0, scal[0], jnp.where(r + m == 65, scal[1], 1))
            hid[at, :] = (v * live.astype(F32)).astype(BF16)
            more[at, :] = skip[at, :] + parts[3 * och :]

    def mix2(y, to):
        to[pl.ds(0, 3 * och), :] = mm(w2[...], window(hid, och, y))

    def end2(y, got):
        for m in range(4):
            v = across(got[:, 128 * m : 128 * m + 128], edge2, y + m, och)
            of[pl.ds(y + m, och, stride=YP), :] = v + more[rows_at(och * (y + m + 1), och, 16), :]

    paired(17, mix1, end1, even, odd)
    paired(16, mix2, end2, even, odd)

    def leave(o, _):
        out[o] = of[rows_at(YP * o, 64, 8), :].astype(BF16)
        return 0

    lax.fori_loop(0, och, leave, 0, unroll=4)


def pick_body(scal, rows, out):
    lon = rows.shape[2]
    for d in range(8):
        hit = chosen(iota((lon, 128), 0) == iota((lon, 128), 1) + scal[8 + d])
        got = mm(rows[scal[d]], hit)
        out[d] = jnp.concatenate([got, jnp.zeros((WP - got.shape[0], 128), F32)], axis=0).astype(BF16)


def call(body, outs, scratch, args, specs=None, scalars=0, flops=10**7, vmem=63):
    def whole(shape):
        zeros = (0,) * len(shape)
        return pl.BlockSpec(shape, lambda i, *_: zeros, pipeline_mode=pl.Buffered(1))

    specs = specs or {}
    return pl.pallas_call(
        body,
        grid_spec=pltpu.PrefetchScalarGridSpec(
            num_scalar_prefetch=scalars,
            grid=(1,),
            in_specs=[specs.get(n) or whole(a.shape) for n, a in enumerate(args[scalars:])],
            out_specs=[whole(o.shape) for o in outs],
            scratch_shapes=scratch,
        ),
        out_shape=outs,
        compiler_params=pltpu.CompilerParams(vmem_limit_bytes=vmem * 2**20),
        cost_estimate=pl.CostEstimate(flops=flops, bytes_accessed=2**20, transcendentals=0),
    )(*args)


def out(shape, dtype=BF16):
    return jax.ShapeDtypeStruct(shape, dtype)


def turned_state(state):
    return call(
        turn_body, [out((64 * SP, 128)), out((4 * SP, 128))],
        [pltpu.VMEM((YP * SP, 128), F32), pltpu.VMEM((512, 128), F32)],
        [state], flops=10**9, vmem=24,
    )


def with_corners(scal, strips, above, below):
    return call(
        corner_body, [out((4 * SP, 128))], [], [scal, strips, above, below],
        scalars=1, vmem=24,
    )[0]


def packed_weights(scal, k1, sw, k2, lon, lat, rho, b1, b2):
    och, cin = sw.shape
    return call(
        pack_body,
        [
            out((4 * och, 3 * SP)), out((3 * och, 3 * SP)), out((4 * och, 3 * CP)),
            out((3 * och, 3 * CP)), out((2, 3 * och, CP)), out((3 * och, 3 * och)),
            out((256, 128)), out((128, 64)), out((och, 128), F32), out((och, 128), F32),
        ],
        [],
        [
            scal, k1.reshape(3, 3 * och, cin), sw, k2.reshape(3, 3 * och, och), lon, lat, rho,
            b1[None], b2[None],
        ],
        specs={
            3: pl.BlockSpec((1, 512, 128), lambda i, s: (s[9], 0, 0)),
            4: pl.BlockSpec((1, 512, 64), lambda i, s: (s[10], 0, 0)),
        },
        scalars=1, flops=10**9,
    )


def early(scal, xs, above, below, ext, west, east, k1, w1s, v1s, wide1, wide2):
    och = k1.shape[2]
    return call(
        early_body,
        [out((68 * och, 128), F32), out((68 * och, 128), F32), out((och, 256), F32)],
        [
            pltpu.VMEM((70 * SP, 128), BF16), pltpu.VMEM((4 * och, 512), F32),
            pltpu.VMEM((4 * och, 512), F32), pltpu.SemaphoreType.DMA,
        ],
        [
            scal, xs, above, below, ext, west, east, k1.reshape(3, 3 * och, -1), w1s, v1s,
            wide1, wide2,
        ],
        specs={0: pl.BlockSpec(memory_space=pltpu.HBM)}, scalars=1, flops=6 * 10**9,
    )


def late(scal, wa, wb, k2, packed, parts):
    acc, skip, side = parts
    w1c, v1c, e1c, w2, lonb, latb = packed[2:8]
    och = side.shape[0]
    vm = pltpu.VMEM
    return call(
        late_body, [out((och, 64, 128))],
        [
            vm((64 * WP, 128), F32), vm((64 * WP, 128), F32), vm((WP * YP, 128), F32),
            vm((128 * CP // 16, 128), F32), vm((70 * CP, 128), BF16), vm((3 * CP, 256), BF16),
            vm((68 * och, 128), BF16), vm((68 * och, 128), F32), vm((68 * och, 128), F32),
            vm((68 * och, 128), F32), vm((2, och, 128), F32), vm((2, och, 128), F32), vm((och * YP, 128), F32),
            vm((4 * och, 512), F32), vm((4 * och, 512), F32), pltpu.SemaphoreType.DMA((2,)),
        ],
        [
            scal, wa, wb, lonb, latb, w1c, v1c, e1c, w2, k2.reshape(3, 3 * och, och), side, acc, skip,
        ],
        specs={10: pl.BlockSpec(memory_space=pltpu.HBM), 11: pl.BlockSpec(memory_space=pltpu.HBM)},
        scalars=1, flops=8 * 10**9,
    )[0]


def picked(scal, rows):
    return call(pick_body, [out((8, WP, 128))], [], [scal, rows], scalars=1, vmem=24)[0]


def totals(mixed, copies):
    return call(total_body, [out((copies, *mixed.shape[1:]))], [], [mixed], vmem=24)[0]


def domain_half(tile, tiles, rotation):
    return ((tile + rotation) % tiles) // (tiles // 2)


def routes(regions, tiles, rotation):
    bands = tiles // ROWS
    half = [[domain_half(ROWS * k + g, tiles, rotation) for k in range(bands)] for g in range(ROWS)]
    by_row, by_domain, rows = [], [], np.zeros((tiles, 2), np.int32)
    for z in range(regions):
        for g in range(ROWS):
            by_row.append([z * tiles + k * ROWS + g for k in range(bands)])
    for g in range(ROWS):
        lower = [k for k in range(bands) if half[g][k] == 0]
        upper = [k for k in range(bands) if half[g][k] == 1]
        for pair in zip(lower, upper):
            by_domain.append([z * tiles + k * ROWS + g for z in range(regions) for k in pair])
            for k in pair:
                rows[k * ROWS + g] = [ROWS * g + pair[0], ROWS * g + pair[1]]
    tile_half = [domain_half(t, tiles, rotation) for t in range(tiles)]
    spread, table = [], np.zeros((2, 2, tiles), np.int32)
    for z in range(regions):
        for h in range(2):
            for core in range(2):
                spread.append([z * tiles + t for t in range(tiles) if tile_half[t] == h and t % 2 == core])
    for h in range(2):
        for core in range(2):
            mine = [t for t in range(tiles) if tile_half[t] == h and t % 2 == core]
            other = [t for t in range(tiles) if tile_half[t] == h and t % 2 != core]
            table[h, core] = np.concatenate([rows[t] for t in mine + other])
    return by_row, by_domain, spread, table


def swap(value, groups):
    return lax.all_to_all(
        value, EVERY, split_axis=0, concat_axis=0, axis_index_groups=groups, tiled=True
    )


def from_neighbour(block, distance):
    size = lax.axis_size("tile")
    return lax.ppermute(block, "tile", [((i - distance) % size, i) for i in range(size)])


def shards(
    global_field,
    regional_state,
    windows,
    longitude_weights,
    latitude_weights,
    first_kernel,
    first_bias,
    second_kernel,
    later_conv_bias,
    shortcut_weight,
):
    tile_count, regions = lax.axis_size("tile"), lax.axis_size("region")
    tile, region = lax.axis_index("tile"), lax.axis_index("region")
    half_count = tile_count // 2
    row_tiles = half_count // TCOLS
    rotation = tile_count // 4 + 2
    position = (tile + rotation) % tile_count
    half, within = position // half_count, position % half_count
    row, col = within // TCOLS, within % TCOLS
    domain = 2 * region + half
    by_row, by_domain, spread, table = routes(regions, tile_count, rotation)

    by_rows = swap(global_field.transpose(1, 0, 2), by_row)

    own = lax.dynamic_index_in_dim(windows, domain, 0, keepdims=False)
    flags = [row > 0, row < row_tiles - 1, col > 0, col < TCOLS - 1]
    scal = jnp.stack([*flags, row, col, own[0], own[1], own[3], domain, half]).astype(jnp.int32)
    rho = lax.dynamic_slice(jnp.asarray(table), (half, tile % 2, 0), (1, 1, 64))[0]

    xs, strips = turned_state(regional_state[0])
    above = from_neighbour(xs[-2 * SP :], TCOLS)
    below = from_neighbour(xs[: 2 * SP], -TCOLS)
    residue = ROWS * (tile % ROWS) + tile // ROWS
    source = (windows[:, 0] + (residue - windows[:, 0]) % 64) // 64
    offset = windows[:, 2] - global_field.shape[2] * region
    where, above, below = lax.optimization_barrier(
        (jnp.concatenate([source, offset]), above, below)
    )
    chosen_parts = picked(where, by_rows)
    ext = with_corners(scal, strips, above, below)
    west = from_neighbour(ext[: 2 * SP], 1)
    east = from_neighbour(ext[2 * SP :], -1)
    packed = packed_weights(
        scal, first_kernel, shortcut_weight, second_kernel, longitude_weights,
        latitude_weights, rho, first_bias, later_conv_bias,
    )
    mixed = swap(chosen_parts, by_domain)
    mixed = mixed.reshape(regions, 2, *mixed.shape[1:])
    mixed, west, east, packed = lax.optimization_barrier((mixed, west, east, packed))
    parts = early(
        scal, xs, above, below, ext, west, east, first_kernel, packed[0], packed[1],
        packed[8], packed[9],
    )
    copies = totals(mixed, len(spread[0]))
    mine = swap(copies, spread)
    mine = mine.reshape(-1, copies.shape[-1])
    other = lax.ppermute(mine, EVERY, [(i, i ^ 1) for i in range(regions * tile_count)])
    return late(scal, mine, other, second_kernel, packed, parts)[None]


def solution(mesh):
    placed = (
        P(None, "tile", "region"),
        P(("region", "tile"), None, None, None),
        P(),
        P(),
        P("region", None, None),
        P(),
        P(),
        P(),
        P(),
        P(),
    )
    return jax.shard_map(
        shards,
        mesh=mesh,
        in_specs=placed,
        out_specs=P(("region", "tile"), None, None, None),
        check_vma=False,
    )
```

```python
import jax
import jax.numpy as jnp
import numpy as np
from jax import lax
from jax.experimental import pallas as pl
from jax.experimental.pallas import tpu as pltpu
from jax.sharding import PartitionSpec as P


TCOLS = 4
ROWS = 8
EVERY = ("region", "tile")
SP = 112
CP = 80
WP = 72
YP = 72
F32, BF16 = jnp.float32, jnp.bfloat16


def mm(a, b):
    return jnp.dot(a, b, preferred_element_type=F32)


def mm_t(a, b):
    return lax.dot_general(a, b, (((1,), (1,)), ((), ())), preferred_element_type=F32)


def iota(shape, dim):
    return lax.broadcasted_iota(jnp.int32, shape, dim)


def chosen(cond):
    return jnp.where(cond, 1.0, 0.0).astype(BF16)


def column(row):
    n = row.shape[1]
    hit = iota((n, n), 0) == iota((n, n), 1)
    return jnp.sum(jnp.where(hit, row, 0.0), axis=1, keepdims=True)


def rows_at(start, size, unit):
    return pl.ds(pl.multiple_of(start, unit), size)


def along(parts, och):
    return (
        parts[:och]
        + pltpu.roll(parts[och : 2 * och], 127, 1)
        + pltpu.roll(parts[2 * och : 3 * och], 126, 1)
    )


CHUNK = 32


def across(parts, m, edges, at, och, k):
    lanes = pl.ds(128 * m, 128)
    lane = iota((CHUNK, 128), 1)
    rows = pl.ds(k, CHUNK)
    west = pltpu.roll(parts[rows, lanes], 1, 1)
    east = pltpu.roll(parts[pl.ds(2 * och + k, CHUNK), lanes], 127, 1)
    west = jnp.where(lane == 0, pltpu.roll(edges[0, rows, :], 128 - at, 1), west)
    east = jnp.where(lane == 127, pltpu.roll(edges[1, rows, :], 127 - at, 1), east)
    return parts[pl.ds(och + k, CHUNK), lanes] + west + east


def stacked(k3, q, och):
    return jnp.concatenate([k3[p, q * och : (q + 1) * och, :] for p in range(3)], axis=0)


def pieces(src, dst, sems, unit):
    moves = []
    for g in range(17):
        at = pl.ds(4 * unit * g, 4 * unit)
        moves.append(
            [
                pltpu.make_async_copy(src[n].at[at, :], dst[n].at[at, :], sems.at[n, g])
                for n in range(2)
            ]
        )
    return moves


def paired(count, mix, end, even, odd):
    hold = (even, odd)
    mix(0, even)
    for g in range(count):
        if g + 1 < count:
            mix(4 * (g + 1), hold[(g + 1) % 2])
        end(4 * g, hold[g % 2])


def turn_body(state, xs, strips, flat, packs):
    chans, height = state.shape[0], state.shape[1]

    def widen(c, _):
        flat[rows_at(YP * c, height, 8), :] = state[c].astype(F32)
        return 0

    lax.fori_loop(0, chans, widen, 0, unroll=3)
    flat[pl.ds(YP * chans, YP * (SP - chans)), :] = jnp.zeros((YP * (SP - chans), 128), F32)

    def row(y, _):
        xs[rows_at(SP * y, SP, 16), :] = flat[pl.ds(y, SP, stride=YP), :].astype(BF16)
        return 0

    lax.fori_loop(0, height, row, 0, unroll=4)
    lane = iota((height, 128), 1)
    for b in range(4):
        packed = jnp.zeros((height, 128), F32)
        for c in range(min(32, chans - 32 * b)):
            one = pltpu.roll(flat[pl.ds(YP * (32 * b + c), height), :], (2 + 4 * c) % 128, 1)
            packed = jnp.where(lane // 4 == c, one, packed)
        packed = jnp.concatenate([packed, jnp.zeros((128 - height, 128), F32)], axis=0)
        packs[pl.ds(128 * b, 128), :] = packed.T
    for col in range(4):
        for b in range(4):
            n = min(32, SP - 32 * b)
            strips[pl.ds(SP * col + 32 * b, n), :] = packs[
                pl.ds(128 * b + col, n, stride=4), :
            ].astype(BF16)


def corner_body(scal, strips, above, below, ext):
    lane = iota((SP, 128), 1)
    top, bottom = scal[0] > 0, scal[1] > 0
    for j, x in enumerate((126, 127, 0, 1)):
        e = pltpu.roll(strips[pl.ds(SP * j, SP), :].astype(F32), 2, 1)
        for m in range(2):
            up = pltpu.roll(above[pl.ds(SP * m, SP), :].astype(F32), (m - x) % 128, 1)
            down = pltpu.roll(below[pl.ds(SP * m, SP), :].astype(F32), (66 + m - x) % 128, 1)
            e = jnp.where((lane == m) & top, up, e)
            e = jnp.where((lane == 66 + m) & bottom, down, e)
        ext[pl.ds(SP * j, SP), :] = e.astype(BF16)


def pack_body(
    scal, k1, sw, k2, lon, lat, rho, b1, b2,
    w1s, v1s, w1c, v1c, e1c, w2, lonb, latb, wide1, wide2,
):
    och, cin = sw.shape
    sch = cin - 70
    wide1[...] = jnp.broadcast_to(column(b1[...]), wide1.shape)
    wide2[...] = jnp.broadcast_to(column(b2[...]), wide2.shape)
    row_s, col_s = iota((cin, 3 * SP), 0), iota((cin, 3 * SP), 1)
    row_c, col_c = iota((cin, 3 * CP), 0), iota((cin, 3 * CP), 1)
    put_s = [chosen((col_s == SP * p + row_s) & (row_s < sch)) for p in range(3)]
    put_c = [chosen((col_c == CP * p + row_c - sch) & (row_c >= sch)) for p in range(3)]
    w1s[pl.ds(0, 3 * och), :] = sum(mm(k1[p], put_s[p]) for p in range(3)).astype(BF16)
    w1s[pl.ds(3 * och, och), :] = mm(sw[...], put_s[1]).astype(BF16)
    w1c[pl.ds(0, 3 * och), :] = sum(mm(k1[p], put_c[p]) for p in range(3)).astype(BF16)
    w1c[pl.ds(3 * och, och), :] = mm(sw[...], put_c[1]).astype(BF16)
    turned = [stacked(k1, q, och) for q in range(3)]
    v1s[...] = sum(mm(turned[q], put_s[q]) for q in range(3)).astype(BF16)
    v1c[...] = sum(mm(turned[q], put_c[q]) for q in range(3)).astype(BF16)
    row_e, col_e = iota((cin, CP), 0), iota((cin, CP), 1)
    put_e = chosen((col_e == row_e - sch) & (row_e >= sch))
    e1c[0] = mm(turned[0], put_e).astype(BF16)
    e1c[1] = mm(turned[2], put_e).astype(BF16)
    row_2, col_2 = iota((och, 3 * och), 0), iota((och, 3 * och), 1)
    w2[...] = sum(mm(k2[p], chosen(col_2 == och * p + row_2)) for p in range(3)).astype(BF16)

    masked = jnp.where(iota((512, 128), 1) < scal[8], lon[0], 0)
    r, c = iota((256, 512), 0), iota((256, 512), 1)
    six = (r - 128) % 8
    off = jnp.where(r < 128, r, jnp.where(six < 3, six - 2, six + 124))
    pick = chosen((c == off + 128 * scal[5]) & ((r < 128) | (six < 6)))
    lonb[...] = mm(pick, masked).astype(BF16)
    r, c = iota((128, 512), 0), iota((128, 512), 1)
    pick = chosen((c == r - 2 + 64 * scal[4]) & (r < 68))
    taken = mm(pick, lat[0]).astype(BF16)
    want = (rho[...] - scal[6]) & 63
    order = chosen((iota((64, 64), 0) == want) & (want < scal[7]))
    latb[...] = mm(taken, order).astype(BF16)


def early_body(
    scal, xs_own, above, below, ext, west, east, k1, w1s, v1s, wide1, wide2,
    acc_far, skip_far, side,
    xs, even, odd, edges, acc, skip, sem, sems,
):
    och = side.shape[0]
    fetch = pltpu.make_async_copy(xs_own, xs.at[pl.ds(2 * SP, 64 * SP)], sem)
    fetch.start()
    top, bottom, left, right = scal[0] > 0, scal[1] > 0, scal[2] > 0, scal[3] > 0
    xs[pl.ds(0, 2 * SP), :] = jnp.where(top, above[...], 0)
    xs[pl.ds(66 * SP, 2 * SP), :] = jnp.where(bottom, below[...], 0)
    xs[pl.ds(68 * SP, 2 * SP), :] = jnp.zeros((2 * SP, 128), BF16)

    west_in = jnp.where(left, west[...], 0)
    east_in = jnp.where(right, east[...], 0)
    ps = jnp.concatenate(
        [
            jnp.concatenate([west_in, ext[pl.ds(2 * SP, SP), :]], axis=0),
            jnp.concatenate([ext[pl.ds(SP, SP), :], east_in], axis=0),
        ],
        axis=1,
    )
    got = mm(v1s[...], ps)
    for s in range(2):
        side[:, 128 * s : 128 * s + 128] = along(got[:, 128 * s : 128 * s + 128], och) + wide1[...]
    edges[0] = along(mm(stacked(k1, 0, och)[:, :SP], west_in[SP:]), och)
    edges[1] = along(mm(stacked(k1, 2, och)[:, :SP], east_in[:SP]), och)
    fetch.wait()

    def mix(r, to):
        rows = [xs[rows_at(SP * (r + m), 3 * SP, 16), :] for m in range(4)]
        to[...] = mm(w1s[...], jnp.concatenate(rows, axis=1))

    def end(r, got):
        for m in range(4):
            for k in range(0, och, CHUNK):
                at = rows_at(och * (r + m) + k, CHUNK, 16)
                rows = pl.ds(k, CHUNK)
                acc[at, :] = across(got, m, edges, r + m, och, k) + wide1[rows, :]
                skip[at, :] = got[pl.ds(3 * och + k, CHUNK), pl.ds(128 * m, 128)] + wide2[rows, :]
        for copy in moves[r // 4]:
            copy.start()

    moves = pieces((acc, skip), (acc_far, skip_far), sems, och)
    paired(17, mix, end, even, odd)
    for pair in moves:
        for copy in pair:
            copy.wait()


def total_body(mixed, out):
    piece = mixed[0].astype(F32)
    for z in range(1, mixed.shape[0]):
        piece = piece + mixed[z].astype(F32)
    piece = piece.astype(BF16)
    for n in range(out.shape[0]):
        out[n] = piece


def late_body(
    scal, wa, wb, lonb, latb, w1c, v1c, e1c, w2, k2, side, acc_far, skip_far,
    out, bands, sideb, cf, ch, cs, pc, hid, acc, skip, more, edge1, edge2, of, even, odd, res, sems, fetched,
):
    och = side.shape[0]
    half = wa.shape[0]
    step = 288
    moves = [
        pltpu.make_async_copy(acc_far, acc, fetched.at[0]),
        pltpu.make_async_copy(skip_far, skip, fetched.at[1]),
    ]
    for copy in moves:
        copy.start()

    def spread(k, _):
        at = pl.multiple_of(k * step, 16)
        for base, part in ((0, wa), (half, wb)):
            got = mm_t(part[pl.ds(at, step), :], lonb[...])
            to = rows_at(base + at, step, 16)
            bands[to, :] = got[:, :128]
            sideb[to, :] = got[:, 128:]
        return 0

    lax.fori_loop(0, half // step, spread, 0)

    def rows(k, _):
        pair = [bands[pl.ds(2 * k + m, 64, stride=WP), :].astype(BF16) for m in range(2)]
        got = mm(latb[pl.ds(0, YP), :], jnp.concatenate(pair, axis=1))
        cf[rows_at(2 * k * YP, YP, 8), :] = got[:, :128]
        cf[rows_at((2 * k + 1) * YP, YP, 8), :] = got[:, 128:]
        return 0

    lax.fori_loop(0, WP // 2, rows, 0, unroll=6)

    lane = iota((64, 128), 1)
    for b in range(CP // 16):
        packed = jnp.zeros((64, 128), F32)
        for c in range(min(16, WP - 16 * b)):
            one = sideb[pl.ds(16 * b + c, 64, stride=WP), :]
            packed = jnp.where(lane // 8 == c, one, packed)
        ch[pl.ds(128 * b, 128), :] = mm_t(packed.T.astype(BF16), latb[...])
    for x in range(6):
        s, k = x // 3, x % 3
        for b in range(CP // 16):
            pc[pl.ds(CP * k + 16 * b, 16), pl.ds(128 * s, 128)] = ch[
                pl.ds(128 * b + x, 16, stride=8), :
            ].astype(BF16)

    def turn(y, _):
        one = cf[pl.ds(y, WP, stride=YP), :]
        one = jnp.concatenate([one, jnp.zeros((CP - WP, 128), F32)], axis=0)
        cs[rows_at(CP * y, CP, 16), :] = one.astype(BF16)
        return 0

    lax.fori_loop(0, 68, turn, 0, unroll=4)
    cs[pl.ds(68 * CP, 2 * CP), :] = jnp.zeros((2 * CP, 128), BF16)

    lane = iota((och, 128), 1)
    got = mm(v1c[...], pc[...])
    for s in range(2):
        lanes = pl.ds(128 * s, 128)
        v = along(got[:, 128 * s : 128 * s + 128], och) + side[:, lanes]
        v = v / (1.0 + jnp.exp(-v))
        keep = (
            ((lane > 0) | (scal[0] > 0))
            & ((lane < 65) | (scal[1] > 0))
            & (lane < 66)
            & (scal[2 + s] > 0)
        )
        v = jnp.where(keep, v, 0.0).astype(BF16)
        edge2[s] = along(mm(stacked(k2, 2 * s, och), v), och)
        edge1[s] = along(mm(e1c[s], pc[pl.ds(CP, CP), lanes]), och)
    for copy in moves:
        copy.wait()

    def window(ref, unit, r):
        return jnp.concatenate(
            [ref[rows_at(unit * (r + m), 3 * unit, 16), :] for m in range(4)], axis=1
        )

    def mix1(r, to):
        to[...] = mm(w1c[...], window(cs, CP, r))

    def end1(r, got):
        for m in range(4):
            live = jnp.where(r + m == 0, scal[0], jnp.where(r + m == 65, scal[1], 1)).astype(F32)
            for k in range(0, och, CHUNK):
                at = rows_at(och * (r + m) + k, CHUNK, 16)
                v = across(got, m, edge1, r + m, och, k) + acc[at, :]
                v = v / (1.0 + jnp.exp(-v))
                hid[at, :] = (v * live).astype(BF16)
                more[at, :] = skip[at, :] + got[pl.ds(3 * och + k, CHUNK), pl.ds(128 * m, 128)]

    def mix2(y, to):
        to[pl.ds(0, 3 * och), :] = mm(w2[...], window(hid, och, y))

    def end2(y, got):
        for m in range(4):
            for k in range(0, och, CHUNK):
                v = across(got, m, edge2, y + m, och, k)
                v = v + more[rows_at(och * (y + m + 1) + k, CHUNK, 16), :]
                of[pl.ds(YP * k + y + m, CHUNK, stride=YP), :] = v
        if y % 16 == 12:
            at = pl.ds(y - 12, 16)
            for o in range(och):
                res[o, at, :] = of[pl.ds(YP * o + y - 12, 16), :].astype(BF16)
            leaves[y // 16].start()

    leaves = [
        pltpu.make_async_copy(
            res.at[:, pl.ds(16 * n, 16), :], out.at[:, pl.ds(16 * n, 16), :], sems.at[n]
        )
        for n in range(4)
    ]
    paired(17, mix1, end1, even, odd)
    paired(16, mix2, end2, even, odd)

    for copy in leaves:
        copy.wait()


def pick_body(scal, rows, out):
    lon = rows.shape[2]
    for d in range(8):
        hit = chosen(iota((lon, 128), 0) == iota((lon, 128), 1) + scal[8 + d])
        got = mm(rows[scal[d]], hit)
        out[d] = jnp.concatenate([got, jnp.zeros((WP - got.shape[0], 128), F32)], axis=0).astype(BF16)


def call(body, outs, scratch, args, specs=None, far=(), scalars=0, flops=10**7, vmem=63):
    def whole(shape):
        zeros = (0,) * len(shape)
        return pl.BlockSpec(shape, lambda i, *_: zeros, pipeline_mode=pl.Buffered(1))

    specs = specs or {}
    return pl.pallas_call(
        body,
        grid_spec=pltpu.PrefetchScalarGridSpec(
            num_scalar_prefetch=scalars,
            grid=(1,),
            in_specs=[specs.get(n) or whole(a.shape) for n, a in enumerate(args[scalars:])],
            out_specs=[
                pl.BlockSpec(memory_space=pltpu.HBM) if n in far else whole(o.shape)
                for n, o in enumerate(outs)
            ],
            scratch_shapes=scratch,
        ),
        out_shape=outs,
        compiler_params=pltpu.CompilerParams(vmem_limit_bytes=vmem * 2**20),
        cost_estimate=pl.CostEstimate(flops=flops, bytes_accessed=2**20, transcendentals=0),
    )(*args)


def out(shape, dtype=BF16):
    return jax.ShapeDtypeStruct(shape, dtype)


def turned_state(state):
    return call(
        turn_body, [out((64 * SP, 128)), out((4 * SP, 128))],
        [pltpu.VMEM((YP * SP, 128), F32), pltpu.VMEM((512, 128), F32)],
        [state], flops=10**9, vmem=24,
    )


def with_corners(scal, strips, above, below):
    return call(
        corner_body, [out((4 * SP, 128))], [], [scal, strips, above, below],
        scalars=1, vmem=24,
    )[0]


def packed_weights(scal, k1, sw, k2, lon, lat, rho, b1, b2):
    och, cin = sw.shape
    return call(
        pack_body,
        [
            out((4 * och, 3 * SP)), out((3 * och, 3 * SP)), out((4 * och, 3 * CP)),
            out((3 * och, 3 * CP)), out((2, 3 * och, CP)), out((3 * och, 3 * och)),
            out((256, 128)), out((128, 64)), out((och, 128), F32), out((och, 128), F32),
        ],
        [],
        [
            scal, k1.reshape(3, 3 * och, cin), sw, k2.reshape(3, 3 * och, och), lon, lat, rho,
            b1[None], b2[None],
        ],
        specs={
            3: pl.BlockSpec((1, 512, 128), lambda i, s: (s[9], 0, 0)),
            4: pl.BlockSpec((1, 512, 64), lambda i, s: (s[10], 0, 0)),
        },
        scalars=1, flops=10**9,
    )


def early(scal, xs, above, below, ext, west, east, k1, w1s, v1s, wide1, wide2):
    och = k1.shape[2]
    return call(
        early_body,
        [out((68 * och, 128), F32), out((68 * och, 128), F32), out((och, 256), F32)],
        [
            pltpu.VMEM((70 * SP, 128), BF16), pltpu.VMEM((4 * och, 512), F32),
            pltpu.VMEM((4 * och, 512), F32), pltpu.VMEM((2, och, 128), F32),
            pltpu.VMEM((68 * och, 128), F32), pltpu.VMEM((68 * och, 128), F32),
            pltpu.SemaphoreType.DMA, pltpu.SemaphoreType.DMA((2, 17)),
        ],
        [
            scal, xs, above, below, ext, west, east, k1.reshape(3, 3 * och, -1), w1s, v1s,
            wide1, wide2,
        ],
        specs={0: pl.BlockSpec(memory_space=pltpu.HBM)}, far=(0, 1), scalars=1, flops=6 * 10**9,
    )


def late(scal, wa, wb, k2, packed, parts):
    acc, skip, side = parts
    w1c, v1c, e1c, w2, lonb, latb = packed[2:8]
    och = side.shape[0]
    vm = pltpu.VMEM
    return call(
        late_body, [out((och, 64, 128))],
        [
            vm((64 * WP, 128), F32), vm((64 * WP, 128), F32), vm((WP * YP, 128), F32),
            vm((128 * CP // 16, 128), F32), vm((70 * CP, 128), BF16), vm((3 * CP, 256), BF16),
            vm((68 * och, 128), BF16), vm((68 * och, 128), F32), vm((68 * och, 128), F32),
            vm((68 * och, 128), F32), vm((2, och, 128), F32), vm((2, och, 128), F32), vm((och * YP, 128), F32),
            vm((4 * och, 512), F32), vm((4 * och, 512), F32), vm((och, 64, 128), BF16),
            pltpu.SemaphoreType.DMA((4,)), pltpu.SemaphoreType.DMA((2,)),
        ],
        [
            scal, wa, wb, lonb, latb, w1c, v1c, e1c, w2, k2.reshape(3, 3 * och, och), side, acc, skip,
        ],
        specs={10: pl.BlockSpec(memory_space=pltpu.HBM), 11: pl.BlockSpec(memory_space=pltpu.HBM)},
        far=(0,), scalars=1, flops=8 * 10**9,
    )[0]


def picked(scal, rows):
    return call(pick_body, [out((8, WP, 128))], [], [scal, rows], scalars=1, vmem=24)[0]


def totals(mixed, copies):
    return call(total_body, [out((copies, *mixed.shape[1:]))], [], [mixed], vmem=24)[0]


def domain_half(tile, tiles, rotation):
    return ((tile + rotation) % tiles) // (tiles // 2)


def routes(regions, tiles, rotation):
    bands = tiles // ROWS
    half = [[domain_half(ROWS * k + g, tiles, rotation) for k in range(bands)] for g in range(ROWS)]
    by_row, by_domain, rows = [], [], np.zeros((tiles, 2), np.int32)
    for z in range(regions):
        for g in range(ROWS):
            by_row.append([z * tiles + k * ROWS + g for k in range(bands)])
    for g in range(ROWS):
        lower = [k for k in range(bands) if half[g][k] == 0]
        upper = [k for k in range(bands) if half[g][k] == 1]
        for pair in zip(lower, upper):
            by_domain.append([z * tiles + k * ROWS + g for z in range(regions) for k in pair])
            for k in pair:
                rows[k * ROWS + g] = [ROWS * g + pair[0], ROWS * g + pair[1]]
    tile_half = [domain_half(t, tiles, rotation) for t in range(tiles)]
    spread, table = [], np.zeros((2, 2, tiles), np.int32)
    for z in range(regions):
        for h in range(2):
            for core in range(2):
                spread.append([z * tiles + t for t in range(tiles) if tile_half[t] == h and t % 2 == core])
    for h in range(2):
        for core in range(2):
            mine = [t for t in range(tiles) if tile_half[t] == h and t % 2 == core]
            other = [t for t in range(tiles) if tile_half[t] == h and t % 2 != core]
            table[h, core] = np.concatenate([rows[t] for t in mine + other])
    return by_row, by_domain, spread, table


def swap(value, groups):
    return lax.all_to_all(
        value, EVERY, split_axis=0, concat_axis=0, axis_index_groups=groups, tiled=True
    )


def from_neighbour(block, distance):
    size = lax.axis_size("tile")
    return lax.ppermute(block, "tile", [((i - distance) % size, i) for i in range(size)])


def shards(
    global_field,
    regional_state,
    windows,
    longitude_weights,
    latitude_weights,
    first_kernel,
    first_bias,
    second_kernel,
    later_conv_bias,
    shortcut_weight,
):
    tile_count, regions = lax.axis_size("tile"), lax.axis_size("region")
    tile, region = lax.axis_index("tile"), lax.axis_index("region")
    half_count = tile_count // 2
    row_tiles = half_count // TCOLS
    rotation = tile_count // 4 + 2
    position = (tile + rotation) % tile_count
    half, within = position // half_count, position % half_count
    row, col = within // TCOLS, within % TCOLS
    domain = 2 * region + half
    by_row, by_domain, spread, table = routes(regions, tile_count, rotation)

    by_rows = swap(global_field.transpose(1, 0, 2), by_row)

    own = lax.dynamic_index_in_dim(windows, domain, 0, keepdims=False)
    flags = [row > 0, row < row_tiles - 1, col > 0, col < TCOLS - 1]
    scal = jnp.stack([*flags, row, col, own[0], own[1], own[3], domain, half]).astype(jnp.int32)
    rho = lax.dynamic_slice(jnp.asarray(table), (half, tile % 2, 0), (1, 1, 64))[0]

    xs, strips = turned_state(regional_state[0])
    above = from_neighbour(xs[-2 * SP :], TCOLS)
    below = from_neighbour(xs[: 2 * SP], -TCOLS)
    residue = ROWS * (tile % ROWS) + tile // ROWS
    source = (windows[:, 0] + (residue - windows[:, 0]) % 64) // 64
    offset = windows[:, 2] - global_field.shape[2] * region
    where, above, below = lax.optimization_barrier(
        (jnp.concatenate([source, offset]), above, below)
    )
    chosen_parts = picked(where, by_rows)
    ext = with_corners(scal, strips, above, below)
    west = from_neighbour(ext[: 2 * SP], 1)
    east = from_neighbour(ext[2 * SP :], -1)
    packed = packed_weights(
        scal, first_kernel, shortcut_weight, second_kernel, longitude_weights,
        latitude_weights, rho, first_bias, later_conv_bias,
    )
    mixed = swap(chosen_parts, by_domain)
    mixed = mixed.reshape(regions, 2, *mixed.shape[1:])
    mixed, west, east, packed = lax.optimization_barrier((mixed, west, east, packed))
    parts = early(
        scal, xs, above, below, ext, west, east, first_kernel, packed[0], packed[1],
        packed[8], packed[9],
    )
    copies = totals(mixed, len(spread[0]))
    mine = swap(copies, spread)
    mine = mine.reshape(-1, copies.shape[-1])
    other = lax.ppermute(mine, EVERY, [(i, i ^ 1) for i in range(regions * tile_count)])
    return late(scal, mine, other, second_kernel, packed, parts)[None]


def solution(mesh):
    placed = (
        P(None, "tile", "region"),
        P(("region", "tile"), None, None, None),
        P(),
        P(),
        P("region", None, None),
        P(),
        P(),
        P(),
        P(),
        P(),
    )
    return jax.shard_map(
        shards,
        mesh=mesh,
        in_specs=placed,
        out_specs=P(("region", "tile"), None, None, None),
        check_vma=False,
    )
```

```python
import jax
import jax.numpy as jnp
import numpy as np
from jax import lax
from jax.experimental import pallas as pl
from jax.experimental.pallas import tpu as pltpu
from jax.sharding import PartitionSpec as P


TCOLS = 4
ROWS = 8
EVERY = ("region", "tile")
SP = 112
CP = 80
WP = 72
YP = 72
F32, BF16 = jnp.float32, jnp.bfloat16


def mm(a, b):
    return jnp.dot(a, b, preferred_element_type=F32)


def mm_t(a, b):
    return lax.dot_general(a, b, (((1,), (1,)), ((), ())), preferred_element_type=F32)


def iota(shape, dim):
    return lax.broadcasted_iota(jnp.int32, shape, dim)


def chosen(cond):
    return jnp.where(cond, 1.0, 0.0).astype(BF16)


def column(row):
    n = row.shape[1]
    hit = iota((n, n), 0) == iota((n, n), 1)
    return jnp.sum(jnp.where(hit, row, 0.0), axis=1, keepdims=True)


def rows_at(start, size, unit):
    return pl.ds(pl.multiple_of(start, unit), size)


def along(parts, och):
    return (
        parts[:och]
        + pltpu.roll(parts[och : 2 * och], 127, 1)
        + pltpu.roll(parts[2 * och : 3 * och], 126, 1)
    )


CHUNK = 32


def across(parts, m, edges, at, och, k):
    lanes = pl.ds(128 * m, 128)
    lane = iota((CHUNK, 128), 1)
    rows = pl.ds(k, CHUNK)
    west = pltpu.roll(parts[rows, lanes], 1, 1)
    east = pltpu.roll(parts[pl.ds(2 * och + k, CHUNK), lanes], 127, 1)
    west = jnp.where(lane == 0, pltpu.roll(edges[0, rows, :], 128 - at, 1), west)
    east = jnp.where(lane == 127, pltpu.roll(edges[1, rows, :], 127 - at, 1), east)
    return parts[pl.ds(och + k, CHUNK), lanes] + west + east


def stacked(k3, q, och):
    return jnp.concatenate([k3[p, q * och : (q + 1) * och, :] for p in range(3)], axis=0)


def pieces(src, dst, sems, unit):
    moves = []
    for g in range(17):
        at = pl.ds(4 * unit * g, 4 * unit)
        moves.append(
            [
                pltpu.make_async_copy(src[n].at[at, :], dst[n].at[at, :], sems.at[n, g])
                for n in range(2)
            ]
        )
    return moves


def paired(count, mix, end, even, odd):
    hold = (even, odd)
    mix(0, even)
    for g in range(count):
        if g + 1 < count:
            mix(4 * (g + 1), hold[(g + 1) % 2])
        end(4 * g, hold[g % 2])


def turn_body(state, xs, strips, flat, packs):
    chans, height = state.shape[0], state.shape[1]

    def widen(c, _):
        flat[rows_at(YP * c, height, 8), :] = state[c].astype(F32)
        return 0

    lax.fori_loop(0, chans, widen, 0, unroll=3)
    flat[pl.ds(YP * chans, YP * (SP - chans)), :] = jnp.zeros((YP * (SP - chans), 128), F32)

    def row(y, _):
        xs[rows_at(SP * y, SP, 16), :] = flat[pl.ds(y, SP, stride=YP), :].astype(BF16)
        return 0

    lax.fori_loop(0, height, row, 0, unroll=4)
    lane = iota((height, 128), 1)
    for b in range(4):
        packed = jnp.zeros((height, 128), F32)
        for c in range(min(32, chans - 32 * b)):
            one = pltpu.roll(flat[pl.ds(YP * (32 * b + c), height), :], (2 + 4 * c) % 128, 1)
            packed = jnp.where(lane // 4 == c, one, packed)
        packed = jnp.concatenate([packed, jnp.zeros((128 - height, 128), F32)], axis=0)
        packs[pl.ds(128 * b, 128), :] = packed.T
    for col in range(4):
        for b in range(4):
            n = min(32, SP - 32 * b)
            strips[pl.ds(SP * col + 32 * b, n), :] = packs[
                pl.ds(128 * b + col, n, stride=4), :
            ].astype(BF16)


def corner_body(scal, strips, above, below, ext):
    lane = iota((SP, 128), 1)
    top, bottom = scal[0] > 0, scal[1] > 0
    for j, x in enumerate((126, 127, 0, 1)):
        e = pltpu.roll(strips[pl.ds(SP * j, SP), :].astype(F32), 2, 1)
        for m in range(2):
            up = pltpu.roll(above[pl.ds(SP * m, SP), :].astype(F32), (m - x) % 128, 1)
            down = pltpu.roll(below[pl.ds(SP * m, SP), :].astype(F32), (66 + m - x) % 128, 1)
            e = jnp.where((lane == m) & top, up, e)
            e = jnp.where((lane == 66 + m) & bottom, down, e)
        ext[pl.ds(SP * j, SP), :] = e.astype(BF16)


def pack_body(
    scal, wins, k1, sw, k2, lon, lat, rho, b1, b2,
    w1s, v1s, w1c, v1c, e1c, w2, lonb, latb, wide1, wide2,
):
    och, cin = sw.shape
    sch = cin - 70
    wide1[...] = jnp.broadcast_to(column(b1[...]), wide1.shape)
    wide2[...] = jnp.broadcast_to(column(b2[...]), wide2.shape)
    row_s, col_s = iota((cin, 3 * SP), 0), iota((cin, 3 * SP), 1)
    row_c, col_c = iota((cin, 3 * CP), 0), iota((cin, 3 * CP), 1)
    put_s = [chosen((col_s == SP * p + row_s) & (row_s < sch)) for p in range(3)]
    put_c = [chosen((col_c == CP * p + row_c - sch) & (row_c >= sch)) for p in range(3)]
    w1s[pl.ds(0, 3 * och), :] = sum(mm(k1[p], put_s[p]) for p in range(3)).astype(BF16)
    w1s[pl.ds(3 * och, och), :] = mm(sw[...], put_s[1]).astype(BF16)
    w1c[pl.ds(0, 3 * och), :] = sum(mm(k1[p], put_c[p]) for p in range(3)).astype(BF16)
    w1c[pl.ds(3 * och, och), :] = mm(sw[...], put_c[1]).astype(BF16)
    turned = [stacked(k1, q, och) for q in range(3)]
    v1s[...] = sum(mm(turned[q], put_s[q]) for q in range(3)).astype(BF16)
    v1c[...] = sum(mm(turned[q], put_c[q]) for q in range(3)).astype(BF16)
    row_e, col_e = iota((cin, CP), 0), iota((cin, CP), 1)
    put_e = chosen((col_e == row_e - sch) & (row_e >= sch))
    e1c[0] = mm(turned[0], put_e).astype(BF16)
    e1c[1] = mm(turned[2], put_e).astype(BF16)
    row_2, col_2 = iota((och, 3 * och), 0), iota((och, 3 * och), 1)
    w2[...] = sum(mm(k2[p], chosen(col_2 == och * p + row_2)) for p in range(3)).astype(BF16)

    mine = scal[6]
    masked = jnp.where(iota((512, 128), 1) < wins[3, mine], lon[0], 0)
    r, c = iota((256, 512), 0), iota((256, 512), 1)
    six = (r - 128) % 8
    off = jnp.where(r < 128, r, jnp.where(six < 3, six - 2, six + 124))
    pick = chosen((c == off + 128 * scal[5]) & ((r < 128) | (six < 6)))
    lonb[...] = mm(pick, masked).astype(BF16)
    r, c = iota((128, 512), 0), iota((128, 512), 1)
    pick = chosen((c == r - 2 + 64 * scal[4]) & (r < 68))
    taken = mm_t(pick, lat[0]).astype(BF16)
    want = (rho[0] - wins[0, mine]) & 63
    order = chosen((iota((64, 64), 0) == want) & (want < wins[1, mine]))
    latb[...] = mm(taken, order).astype(BF16)


def early_body(
    scal, xs_own, above, below, ext, west, east, k1, w1s, v1s, wide1, wide2,
    acc_far, skip_far, side,
    xs, even, odd, edges, acc, skip, sem, sems,
):
    och = side.shape[0]
    fetch = pltpu.make_async_copy(xs_own, xs.at[pl.ds(2 * SP, 64 * SP)], sem)
    fetch.start()
    top, bottom, left, right = scal[0] > 0, scal[1] > 0, scal[2] > 0, scal[3] > 0
    xs[pl.ds(0, 2 * SP), :] = jnp.where(top, above[...], 0)
    xs[pl.ds(66 * SP, 2 * SP), :] = jnp.where(bottom, below[...], 0)
    xs[pl.ds(68 * SP, 2 * SP), :] = jnp.zeros((2 * SP, 128), BF16)

    west_in = jnp.where(left, west[...], 0)
    east_in = jnp.where(right, east[...], 0)
    ps = jnp.concatenate(
        [
            jnp.concatenate([west_in, ext[pl.ds(2 * SP, SP), :]], axis=0),
            jnp.concatenate([ext[pl.ds(SP, SP), :], east_in], axis=0),
        ],
        axis=1,
    )
    got = mm(v1s[...], ps)
    for s in range(2):
        side[:, 128 * s : 128 * s + 128] = along(got[:, 128 * s : 128 * s + 128], och) + wide1[...]
    edges[0] = along(mm(stacked(k1, 0, och)[:, :SP], west_in[SP:]), och)
    edges[1] = along(mm(stacked(k1, 2, och)[:, :SP], east_in[:SP]), och)
    fetch.wait()

    def mix(r, to):
        rows = [xs[rows_at(SP * (r + m), 3 * SP, 16), :] for m in range(4)]
        to[...] = mm(w1s[...], jnp.concatenate(rows, axis=1))

    def end(r, got):
        for m in range(4):
            for k in range(0, och, CHUNK):
                at = rows_at(och * (r + m) + k, CHUNK, 16)
                rows = pl.ds(k, CHUNK)
                acc[at, :] = across(got, m, edges, r + m, och, k) + wide1[rows, :]
                skip[at, :] = got[pl.ds(3 * och + k, CHUNK), pl.ds(128 * m, 128)] + wide2[rows, :]
        for copy in moves[r // 4]:
            copy.start()

    moves = pieces((acc, skip), (acc_far, skip_far), sems, och)
    paired(17, mix, end, even, odd)
    for pair in moves:
        for copy in pair:
            copy.wait()


def total_body(mixed, out):
    piece = mixed[0].astype(F32)
    for z in range(1, mixed.shape[0]):
        piece = piece + mixed[z].astype(F32)
    piece = piece.astype(BF16)
    for n in range(out.shape[0]):
        out[n] = piece


def late_body(
    scal, wa, wb, lonb, latb, w1c, v1c, e1c, w2, k2, side, acc_far, skip_far,
    out, bands, sideb, cf, ch, cs, pc, hid, acc, skip, more, edge1, edge2, of, even, odd, res, sems, fetched,
):
    och = side.shape[0]
    half = wa.shape[0]
    step = 288
    moves = [
        pltpu.make_async_copy(acc_far, acc, fetched.at[0]),
        pltpu.make_async_copy(skip_far, skip, fetched.at[1]),
    ]
    for copy in moves:
        copy.start()

    def spread(k, _):
        at = pl.multiple_of(k * step, 16)
        for base, part in ((0, wa), (half, wb)):
            got = mm_t(part[pl.ds(at, step), :], lonb[...])
            to = rows_at(base + at, step, 16)
            bands[to, :] = got[:, :128]
            sideb[to, :] = got[:, 128:]
        return 0

    lax.fori_loop(0, half // step, spread, 0)

    def rows(k, _):
        pair = [bands[pl.ds(2 * k + m, 64, stride=WP), :].astype(BF16) for m in range(2)]
        got = mm(latb[pl.ds(0, YP), :], jnp.concatenate(pair, axis=1))
        cf[rows_at(2 * k * YP, YP, 8), :] = got[:, :128]
        cf[rows_at((2 * k + 1) * YP, YP, 8), :] = got[:, 128:]
        return 0

    lax.fori_loop(0, WP // 2, rows, 0, unroll=6)

    lane = iota((64, 128), 1)
    for b in range(CP // 16):
        packed = jnp.zeros((64, 128), F32)
        for c in range(min(16, WP - 16 * b)):
            one = sideb[pl.ds(16 * b + c, 64, stride=WP), :]
            packed = jnp.where(lane // 8 == c, one, packed)
        ch[pl.ds(128 * b, 128), :] = mm_t(packed.T.astype(BF16), latb[...])
    for x in range(6):
        s, k = x // 3, x % 3
        for b in range(CP // 16):
            pc[pl.ds(CP * k + 16 * b, 16), pl.ds(128 * s, 128)] = ch[
                pl.ds(128 * b + x, 16, stride=8), :
            ].astype(BF16)

    def turn(y, _):
        one = cf[pl.ds(y, WP, stride=YP), :]
        one = jnp.concatenate([one, jnp.zeros((CP - WP, 128), F32)], axis=0)
        cs[rows_at(CP * y, CP, 16), :] = one.astype(BF16)
        return 0

    lax.fori_loop(0, 68, turn, 0, unroll=4)
    cs[pl.ds(68 * CP, 2 * CP), :] = jnp.zeros((2 * CP, 128), BF16)

    lane = iota((och, 128), 1)
    got = mm(v1c[...], pc[...])
    for s in range(2):
        lanes = pl.ds(128 * s, 128)
        v = along(got[:, 128 * s : 128 * s + 128], och) + side[:, lanes]
        v = v / (1.0 + jnp.exp(-v))
        keep = (
            ((lane > 0) | (scal[0] > 0))
            & ((lane < 65) | (scal[1] > 0))
            & (lane < 66)
            & (scal[2 + s] > 0)
        )
        v = jnp.where(keep, v, 0.0).astype(BF16)
        edge2[s] = along(mm(stacked(k2, 2 * s, och), v), och)
        edge1[s] = along(mm(e1c[s], pc[pl.ds(CP, CP), lanes]), och)
    for copy in moves:
        copy.wait()

    def window(ref, unit, r):
        return jnp.concatenate(
            [ref[rows_at(unit * (r + m), 3 * unit, 16), :] for m in range(4)], axis=1
        )

    def mix1(r, to):
        to[...] = mm(w1c[...], window(cs, CP, r))

    def end1(r, got):
        for m in range(4):
            live = jnp.where(r + m == 0, scal[0], jnp.where(r + m == 65, scal[1], 1)).astype(F32)
            for k in range(0, och, CHUNK):
                at = rows_at(och * (r + m) + k, CHUNK, 16)
                v = across(got, m, edge1, r + m, och, k) + acc[at, :]
                v = v / (1.0 + jnp.exp(-v))
                hid[at, :] = (v * live).astype(BF16)
                more[at, :] = skip[at, :] + got[pl.ds(3 * och + k, CHUNK), pl.ds(128 * m, 128)]

    def mix2(y, to):
        to[pl.ds(0, 3 * och), :] = mm(w2[...], window(hid, och, y))

    def end2(y, got):
        for m in range(4):
            for k in range(0, och, CHUNK):
                v = across(got, m, edge2, y + m, och, k)
                v = v + more[rows_at(och * (y + m + 1) + k, CHUNK, 16), :]
                of[pl.ds(YP * k + y + m, CHUNK, stride=YP), :] = v
        if y % 16 == 12:
            at = pl.ds(y - 12, 16)
            for o in range(och):
                res[o, at, :] = of[pl.ds(YP * o + y - 12, 16), :].astype(BF16)
            leaves[y // 16].start()

    leaves = [
        pltpu.make_async_copy(
            res.at[:, pl.ds(16 * n, 16), :], out.at[:, pl.ds(16 * n, 16), :], sems.at[n]
        )
        for n in range(4)
    ]
    paired(17, mix1, end1, even, odd)
    paired(16, mix2, end2, even, odd)

    for copy in leaves:
        copy.wait()


def pick_body(scal, wins, rows, out):
    lon = rows.shape[2]
    for d in range(8):
        start = wins[0, d]
        source = (start + ((scal[9] - start) & 63)) >> 6
        hit = chosen(iota((lon, 128), 0) == iota((lon, 128), 1) + (wins[2, d] - lon * scal[10]))
        got = mm(rows[source], hit)
        out[d] = jnp.concatenate([got, jnp.zeros((WP - got.shape[0], 128), F32)], axis=0).astype(BF16)


def call(body, outs, scratch, args, specs=None, far=(), scalars=0, flops=10**7, vmem=63):
    def whole(shape):
        zeros = (0,) * len(shape)
        return pl.BlockSpec(shape, lambda i, *_: zeros, pipeline_mode=pl.Buffered(1))

    specs = specs or {}
    return pl.pallas_call(
        body,
        grid_spec=pltpu.PrefetchScalarGridSpec(
            num_scalar_prefetch=scalars,
            grid=(1,),
            in_specs=[specs.get(n) or whole(a.shape) for n, a in enumerate(args[scalars:])],
            out_specs=[
                pl.BlockSpec(memory_space=pltpu.HBM) if n in far else whole(o.shape)
                for n, o in enumerate(outs)
            ],
            scratch_shapes=scratch,
        ),
        out_shape=outs,
        compiler_params=pltpu.CompilerParams(vmem_limit_bytes=vmem * 2**20),
        cost_estimate=pl.CostEstimate(flops=flops, bytes_accessed=2**20, transcendentals=0),
    )(*args)


def out(shape, dtype=BF16):
    return jax.ShapeDtypeStruct(shape, dtype)


def turned_state(state):
    return call(
        turn_body, [out((64 * SP, 128)), out((4 * SP, 128))],
        [pltpu.VMEM((YP * SP, 128), F32), pltpu.VMEM((512, 128), F32)],
        [state], flops=10**9, vmem=24,
    )


def with_corners(scal, strips, above, below):
    return call(
        corner_body, [out((4 * SP, 128))], [], [scal, strips, above, below],
        scalars=1, vmem=24,
    )[0]


def packed_weights(scal, wins, k1, sw, k2, lon, lat, rho, b1, b2):
    och, cin = sw.shape
    return call(
        pack_body,
        [
            out((4 * och, 3 * SP)), out((3 * och, 3 * SP)), out((4 * och, 3 * CP)),
            out((3 * och, 3 * CP)), out((2, 3 * och, CP)), out((3 * och, 3 * och)),
            out((256, 128)), out((128, 64)), out((och, 128), F32), out((och, 128), F32),
        ],
        [],
        [
            scal, wins, k1.reshape(3, 3 * och, cin), sw, k2.reshape(3, 3 * och, och), lon,
            lat.transpose(0, 2, 1), rho, b1[None], b2[None],
        ],
        specs={
            3: pl.BlockSpec((1, 512, 128), lambda i, s, w: (s[6], 0, 0)),
            4: pl.BlockSpec((1, 64, 512), lambda i, s, w: (s[7], 0, 0)),
            5: pl.BlockSpec((1, 1, 64), lambda i, s, w: (s[8], 0, 0)),
        },
        scalars=2, flops=10**9,
    )


def early(scal, xs, above, below, ext, west, east, k1, w1s, v1s, wide1, wide2):
    och = k1.shape[2]
    return call(
        early_body,
        [out((68 * och, 128), F32), out((68 * och, 128), F32), out((och, 256), F32)],
        [
            pltpu.VMEM((70 * SP, 128), BF16), pltpu.VMEM((4 * och, 512), F32),
            pltpu.VMEM((4 * och, 512), F32), pltpu.VMEM((2, och, 128), F32),
            pltpu.VMEM((68 * och, 128), F32), pltpu.VMEM((68 * och, 128), F32),
            pltpu.SemaphoreType.DMA, pltpu.SemaphoreType.DMA((2, 17)),
        ],
        [
            scal, xs, above, below, ext, west, east, k1.reshape(3, 3 * och, -1), w1s, v1s,
            wide1, wide2,
        ],
        specs={0: pl.BlockSpec(memory_space=pltpu.HBM)}, far=(0, 1), scalars=1, flops=6 * 10**9,
    )


def late(scal, wa, wb, k2, packed, parts):
    acc, skip, side = parts
    w1c, v1c, e1c, w2, lonb, latb = packed[2:8]
    och = side.shape[0]
    vm = pltpu.VMEM
    return call(
        late_body, [out((och, 64, 128))],
        [
            vm((64 * WP, 128), F32), vm((64 * WP, 128), F32), vm((WP * YP, 128), F32),
            vm((128 * CP // 16, 128), F32), vm((70 * CP, 128), BF16), vm((3 * CP, 256), BF16),
            vm((68 * och, 128), BF16), vm((68 * och, 128), F32), vm((68 * och, 128), F32),
            vm((68 * och, 128), F32), vm((2, och, 128), F32), vm((2, och, 128), F32), vm((och * YP, 128), F32),
            vm((4 * och, 512), F32), vm((4 * och, 512), F32), vm((och, 64, 128), BF16),
            pltpu.SemaphoreType.DMA((4,)), pltpu.SemaphoreType.DMA((2,)),
        ],
        [
            scal, wa, wb, lonb, latb, w1c, v1c, e1c, w2, k2.reshape(3, 3 * och, och), side, acc, skip,
        ],
        specs={10: pl.BlockSpec(memory_space=pltpu.HBM), 11: pl.BlockSpec(memory_space=pltpu.HBM)},
        far=(0,), scalars=1, flops=8 * 10**9,
    )[0]


def picked(scal, wins, rows):
    return call(pick_body, [out((8, WP, 128))], [], [scal, wins, rows], scalars=2, vmem=24)[0]


def totals(mixed, copies):
    return call(total_body, [out((copies, *mixed.shape[1:]))], [], [mixed], vmem=24)[0]


def domain_half(tile, tiles, rotation):
    return ((tile + rotation) % tiles) // (tiles // 2)


def routes(regions, tiles, rotation):
    bands = tiles // ROWS
    half = [[domain_half(ROWS * k + g, tiles, rotation) for k in range(bands)] for g in range(ROWS)]
    by_row, by_domain, rows = [], [], np.zeros((tiles, 2), np.int32)
    for z in range(regions):
        for g in range(ROWS):
            by_row.append([z * tiles + k * ROWS + g for k in range(bands)])
    for g in range(ROWS):
        lower = [k for k in range(bands) if half[g][k] == 0]
        upper = [k for k in range(bands) if half[g][k] == 1]
        for pair in zip(lower, upper):
            by_domain.append([z * tiles + k * ROWS + g for z in range(regions) for k in pair])
            for k in pair:
                rows[k * ROWS + g] = [ROWS * g + pair[0], ROWS * g + pair[1]]
    tile_half = [domain_half(t, tiles, rotation) for t in range(tiles)]
    spread, table = [], np.zeros((2, 2, tiles), np.int32)
    for z in range(regions):
        for h in range(2):
            for core in range(2):
                spread.append([z * tiles + t for t in range(tiles) if tile_half[t] == h and t % 2 == core])
    for h in range(2):
        for core in range(2):
            mine = [t for t in range(tiles) if tile_half[t] == h and t % 2 == core]
            other = [t for t in range(tiles) if tile_half[t] == h and t % 2 != core]
            table[h, core] = np.concatenate([rows[t] for t in mine + other])
    place = np.zeros((regions * tiles, 16), np.int32)
    for z in range(regions):
        for t in range(tiles):
            within = (t + rotation) % tiles % (tiles // 2)
            row, col = within // TCOLS, within % TCOLS
            edges = [row > 0, row < tiles // 2 // TCOLS - 1, col > 0, col < TCOLS - 1]
            half_at = tile_half[t]
            place[z * tiles + t, :11] = [
                *edges, row, col, 2 * z + half_at, half_at, 2 * half_at + t % 2,
                ROWS * (t % ROWS) + t // ROWS, z,
            ]
    return by_row, by_domain, spread, table, place


def swap(value, groups):
    return lax.all_to_all(
        value, EVERY, split_axis=0, concat_axis=0, axis_index_groups=groups, tiled=True
    )


def from_neighbour(block, distance):
    size = lax.axis_size("tile")
    return lax.ppermute(block, "tile", [((i - distance) % size, i) for i in range(size)])


def shards(
    global_field,
    regional_state,
    windows,
    longitude_weights,
    latitude_weights,
    first_kernel,
    first_bias,
    second_kernel,
    later_conv_bias,
    shortcut_weight,
):
    tile_count, regions = lax.axis_size("tile"), lax.axis_size("region")
    tile, region = lax.axis_index("tile"), lax.axis_index("region")
    rotation = tile_count // 4 + 2
    by_row, by_domain, spread, table, place = routes(regions, tile_count, rotation)

    by_rows = swap(global_field.transpose(1, 0, 2), by_row)

    device = region * tile_count + tile
    scal = lax.dynamic_slice(jnp.asarray(place), (device, 0), (1, place.shape[1]))[0]
    wins = windows.T

    xs, strips = turned_state(regional_state[0])
    above = from_neighbour(xs[-2 * SP :], TCOLS)
    below = from_neighbour(xs[: 2 * SP], -TCOLS)
    chooser, above, below = lax.optimization_barrier((scal, above, below))
    chosen_parts = picked(chooser, wins, by_rows)
    ext = with_corners(scal, strips, above, below)
    packed = packed_weights(
        scal, wins, first_kernel, shortcut_weight, second_kernel, longitude_weights,
        latitude_weights, jnp.asarray(table.reshape(4, 1, -1)), first_bias, later_conv_bias,
    )
    ext, packed = lax.optimization_barrier((ext, packed))
    west = from_neighbour(ext[: 2 * SP], 1)
    east = from_neighbour(ext[2 * SP :], -1)
    mixed = swap(chosen_parts, by_domain)
    mixed = mixed.reshape(regions, 2, *mixed.shape[1:])
    parts = early(
        scal, xs, above, below, ext, west, east, first_kernel, packed[0], packed[1],
        packed[8], packed[9],
    )
    copies = totals(mixed, len(spread[0]))
    mine = swap(copies, spread)
    mine = mine.reshape(-1, copies.shape[-1])
    other = lax.ppermute(mine, EVERY, [(i, i ^ 1) for i in range(regions * tile_count)])
    return late(scal, mine, other, second_kernel, packed, parts)[None]


def solution(mesh):
    placed = (
        P(None, "tile", "region"),
        P(("region", "tile"), None, None, None),
        P(),
        P(),
        P("region", None, None),
        P(),
        P(),
        P(),
        P(),
        P(),
    )
    return jax.shard_map(
        shards,
        mesh=mesh,
        in_specs=placed,
        out_specs=P(("region", "tile"), None, None, None),
        check_vma=False,
    )
```
